128 devices in a mesh: dp: 4 (over z), row: 8 (over x_lo, y), col: 4 (over x_hi, core).
Axes of the slice: x: 4 (x_hi: 2, x_lo: 2; x = x_hi * 2 + x_lo), y: 4, z: 4, core: 2. Of those that a mesh axis runs over, the one named last changes fastest.
Arguments:
- tokens: bfloat16 [32768, 6144], P(('dp', 'row', 'col')), may hold values from -60 to 60
- grads: bfloat16 [32768, 24576], P(('dp', 'row', 'col')), may hold values from -2 to 2
- weight_grad: bfloat16 [6144, 24576], P('row', ('dp', 'col')), may hold values from -0.5 to 0.5
Outputs:
- update: bfloat16 [6144, 24576], P('row', ('dp', 'col'))
The draws below stay inside these ranges and needn't reach their ends.
All inputs are finite; a program needn't handle non-finite values.
Results may differ from the reference program's by a relative error of at most 0.00065.
The reference program's roundings to bfloat16 on the way (of `inverse_in`, `inverse_out` and `left`) count: a program that leaves them out, or rounds other values in their place, can miss the bound.
Values may be sent and summed in bfloat16 or wider, within the bound.
No kernel may reach another device: no remote copies, remote signals or barrier semaphores. Data moves between devices by JAX's collectives and lax.ppermute only.
A program may use at most 192 MiB of HBM per device.

```python
import math
import jax
import jax.numpy as jnp
from jax import lax

D = 6144
F = 24576
BLOCK = 192
STEPS = 3
TOKENS = 32768


def scaled_field(key, rows, cols, base, row_trend, col_trend, loose_columns):
    keys = jax.random.split(key, 5)
    row_pos = jnp.arange(rows, dtype=jnp.float32) / rows
    col_pos = jnp.arange(cols, dtype=jnp.float32) / cols
    row_scale = 10.0 ** (row_trend * row_pos) * jnp.exp(jax.random.uniform(keys[0], (rows,), jnp.float32, -0.35, 0.35))
    if loose_columns:
        col_scale = jnp.exp(jax.random.uniform(keys[1], (cols,), jnp.float32, jnp.log(0.3), jnp.log(3.0)))
    else:
        col_scale = 10.0 ** (col_trend * col_pos) * jnp.exp(jax.random.uniform(keys[1], (cols,), jnp.float32, -0.35, 0.35))
    noise = jax.random.truncated_normal(keys[4], -4.0, 4.0, (rows, cols), jnp.float32)
    return base * noise * row_scale[:, None] * col_scale[None, :]


def draw_tokens(key, part):
    return scaled_field(jax.random.fold_in(key, 11), TOKENS, D, 1.0 / 3.0, 1.0, 0.0, True).astype(jnp.bfloat16)


def draw_grads(key, part):
    base = 0.02 / 3.0
    return scaled_field(jax.random.fold_in(key, 23), TOKENS, F, base, 1.0, 0.0, True).astype(jnp.bfloat16)


def draw_weight_grad(key, part):
    base = 0.005
    return scaled_field(jax.random.fold_in(key, 37), D, F, base, 0.5, 0.5, False).astype(jnp.bfloat16)


def setup_inputs(seed: int = 0) -> dict:
    splits = jax.random.split(jax.random.key(seed), 4)
    return {
        "tokens": draw_tokens(jax.random.fold_in(splits[3], 71), 0),
        "grads": draw_grads(jax.random.fold_in(splits[3], 71), 0),
        "weight_grad": draw_weight_grad(jax.random.fold_in(splits[3], 71), 0),
    }


epsilon = 1e-06
damping = 0.01
trust_radius = 0.05
highest = lax.Precision.HIGHEST

def newton_inverse(blocks, shift):
    size = blocks.shape[-1]
    identity = jnp.eye(size, dtype=jnp.float32)
    matrix = blocks + shift * identity
    frobenius = jnp.sqrt(lax.optimization_barrier(jnp.sum(matrix * matrix, axis=(1, 2))))
    iterate = identity[None, :, :] / frobenius[:, None, None]
    for sweep in range(STEPS):
        product = jnp.einsum('nij,njk->nik', matrix, iterate, precision=highest)
        iterate = jnp.einsum('nij,njk->nik', iterate, 2.0 * identity - product, precision=highest)
    return iterate.astype(jnp.bfloat16)

def covariance(data):
    total = data.shape[0]
    count_blocks = data.shape[1] // BLOCK
    rows_step = math.gcd(total, 1024)

    def accumulate(index, summed):
        piece = lax.dynamic_slice_in_dim(data, index * rows_step, rows_step, 0)
        piece = piece.astype(jnp.float32).reshape(rows_step, count_blocks, BLOCK)
        return summed + jnp.einsum('tai,taj->aij', piece, piece, precision=highest)
    start = jnp.zeros((count_blocks, BLOCK, BLOCK), jnp.float32)
    return lax.fori_loop(0, total // rows_step, accumulate, start) / total

def block_trace(blocks):
    return jnp.sum(jnp.diagonal(blocks, axis1=1, axis2=2))

def reference(tokens, grads, weight_grad):
    cov_in = covariance(tokens)
    cov_out = covariance(grads)
    trace_in = block_trace(cov_in)
    trace_out = block_trace(cov_out)
    ratio = jnp.sqrt((trace_in / D + epsilon) / (trace_out / F + epsilon))
    damp_root = math.sqrt(damping)
    inverse_in = newton_inverse(cov_in, ratio * damp_root)
    inverse_out = newton_inverse(cov_out, damp_root / ratio)
    shaped = weight_grad.astype(jnp.float32).reshape(D // BLOCK, BLOCK, F)
    left = jnp.einsum('aij,ajc->aic', inverse_in.astype(jnp.float32), shaped, precision=highest)
    left = left.reshape(D, F).astype(jnp.bfloat16)
    natural = jnp.einsum('rkj,kji->rki', left.astype(jnp.float32).reshape(D, F // BLOCK, BLOCK), inverse_out.astype(jnp.float32), precision=highest).reshape(D, F)
    alignment = jnp.sum(natural * weight_grad.astype(jnp.float32))
    return (natural * jnp.sqrt(trust_radius * D * F / alignment)).astype(jnp.bfloat16)
```

```python
import functools
import math

import jax
import jax.numpy as jnp
from jax import lax
from jax.experimental import pallas as pl
from jax.experimental.pallas import tpu as pltpu
from jax.sharding import Mesh
from jax.sharding import PartitionSpec as P

D = 6144
F = 24576
TOKENS = 32768
BLOCK = 192
STEPS = 3
ALL = ("dp", "row_0", "row_1", "col_0", "col_1")
ROW = ("row_0", "row_1")
DP_COL = ("dp", "col_0", "col_1")

epsilon = 1e-06
damping = 0.01
trust_radius = 0.05


X_MASKS = (0, 16, 2, 18)
Y_MASKS = (0, 4, 8, 12)
Z_MASKS = (0, 32, 64, 96)
CORE_MASKS = (0, 1)
HALF = BLOCK // 3
LANES = 128


def swap(array, mask):
    return lax.ppermute(array, ALL, [(i, i ^ mask) for i in range(128)])


def all_sum(value):
    for masks in (CORE_MASKS, X_MASKS, Y_MASKS, Z_MASKS):
        value = value + sum(swap(value, mask) for mask in masks[1:])
    return value


def packed_pair(pair_own, pair_got, first):
    even = jnp.zeros((BLOCK, 256), jnp.float32)
    odd = jnp.zeros((BLOCK, 256), jnp.float32)
    for part in (pair_own, pair_got):
        turned = part.T
        even += jnp.dot(turned[:BLOCK], part[:, :256], preferred_element_type=jnp.float32)
        odd += jnp.dot(turned[BLOCK:], part[:, 128:], preferred_element_type=jnp.float32)
    low = lax.broadcasted_iota(jnp.int32, (HALF, LANES), 1) < HALF
    e = [[even[HALF * i : HALF * (i + 1), LANES * j : LANES * (j + 1)] for j in range(2)] for i in range(3)]
    o = [[odd[HALF * i : HALF * (i + 1), LANES * j : LANES * (j + 1)] for j in range(2)] for i in range(3)]
    evens = (e[0][0], jnp.where(low, e[0][1], e[1][0]), jnp.where(low, e[2][1], e[2][0]))
    odds = (jnp.where(low, o[0][1], o[0][0]), jnp.where(low, o[1][1], o[0][1]), o[2][1])
    picked = []
    for bit in range(2):
        same = first == 0
        one, two = (evens, odds) if bit == 0 else (odds, evens)
        picked.append([jnp.where(same, a, b) for a, b in zip(one, two)])
    return picked


def out_kernel(where, own, got, *outs):
    a_outs, b_outs, c_out = outs[:4], outs[4:8], outs[8]
    step = pl.program_id(0)
    place = where[8]
    for high in range(2):
        offset = pl.multiple_of((high ^ (place // 2)) * 384, 384)
        pieces = packed_pair(own[:, pl.ds(offset, 384)], got[:, pl.ds(offset, 384)], lax.rem(place, 2))
        for bit in range(2):
            slot = 2 * high + bit
            first, second, third = pieces[bit]
            for k in range(4):

                @pl.when(step == k)
                def _(k=k):
                    a_outs[k][slot] = first

            b_outs[slot][step] = second
            c_out[step, slot] = third


def out_blocks(where, own, got):
    small = jax.ShapeDtypeStruct((4, HALF, LANES), jnp.float32)
    big = jax.ShapeDtypeStruct((4, 4, HALF, LANES), jnp.float32)
    whole = pl.BlockSpec((4, HALF, LANES), lambda i, w: (0, 0, 0))
    return pl.pallas_call(
        out_kernel,
        grid_spec=pltpu.PrefetchScalarGridSpec(
            num_scalar_prefetch=1,
            grid=(4,),
            in_specs=[
                pl.BlockSpec((256, 768), lambda i, w: (0, w[i])),
                pl.BlockSpec((256, 768), lambda i, w: (0, w[4 + i])),
            ],
            out_specs=[whole] * 8 + [pl.BlockSpec((4, 4, HALF, LANES), lambda i, w: (0, 0, 0, 0))],
        ),
        out_shape=[small] * 8 + [big],
        cost_estimate=pl.CostEstimate(flops=5_000_000_000, bytes_accessed=5_000_000, transcendentals=0),
        compiler_params=pltpu.CompilerParams(vmem_limit_bytes=24 * 1024 * 1024),
        name="cov_out",
    )(where, own, got)


def in_kernel(where, own, got, *outs):
    a_outs, b_outs = outs[:4], outs[4:]
    step = pl.program_id(0)
    place = where[8]
    for high in range(2):
        offset = pl.multiple_of((high ^ (place // 2)) * 384, 384)
        pieces = packed_pair(own[:, pl.ds(offset, 384)], got[:, pl.ds(offset, 384)], lax.rem(place, 2))
        for bit in range(2):
            slot = 2 * high + bit
            first, second, third = pieces[bit]
            for k in range(4):

                @pl.when(step == k)
                def _(k=k):
                    a_outs[k][slot, :64] = first
                    a_outs[k][slot, 64:] = second[:32]

            b_outs[slot][step, :64] = third
            b_outs[slot][step, 64:] = second[32:]


def in_blocks(where, own, got):
    small = jax.ShapeDtypeStruct((4, 96, LANES), jnp.float32)
    whole = pl.BlockSpec((4, 96, LANES), lambda i, w: (0, 0, 0))
    return pl.pallas_call(
        in_kernel,
        grid_spec=pltpu.PrefetchScalarGridSpec(
            num_scalar_prefetch=1,
            grid=(4,),
            in_specs=[
                pl.BlockSpec((256, 768), lambda i, w: (0, w[i])),
                pl.BlockSpec((256, 768), lambda i, w: (0, w[4 + i])),
            ],
            out_specs=[whole] * 8,
        ),
        out_shape=[small] * 8,
        cost_estimate=pl.CostEstimate(flops=5_000_000_000, bytes_accessed=5_000_000, transcendentals=0),
        compiler_params=pltpu.CompilerParams(vmem_limit_bytes=24 * 1024 * 1024),
        name="cov_in",
    )(where, own, got)


def inverse_kernel(flag, shift, first, second, third, out):
    swapped = flag[0] == 1
    c = []
    for piece in (first, second, third):
        value = piece[...]
        c.append(jnp.where(swapped, pltpu.roll(value, HALF, 1), value))
    t = [jnp.concatenate([value, value], axis=0).T for value in c]
    low = lax.broadcasted_iota(jnp.int32, (HALF, LANES), 1) < HALF
    zero = jnp.zeros((HALF, LANES), jnp.float32)
    rows = [
        [c[0], jnp.where(low, c[1], zero)],
        [jnp.where(low, t[0][HALF:], c[1]), jnp.where(low, t[2][HALF:], zero)],
        [jnp.where(low, t[1][:HALF], c[2]), jnp.where(low, c[2], zero)],
        [zero, zero],
    ]
    blocks = jnp.concatenate([jnp.concatenate(pair, axis=1) for pair in rows], axis=0)
    i = lax.broadcasted_iota(jnp.int32, (256, 256), 0)
    j = lax.broadcasted_iota(jnp.int32, (256, 256), 1)
    identity = jnp.where((i == j) & (i < BLOCK), 1.0, 0.0).astype(jnp.float32)
    matrix = blocks * (1.0 / TOKENS) + shift[0] * identity
    squares = jnp.sum(matrix * matrix, axis=(0, 1), keepdims=True)
    iterate = identity / jnp.sqrt(squares)
    for sweep in range(STEPS):
        product = jnp.dot(matrix, iterate, precision=lax.Precision.HIGHEST, preferred_element_type=jnp.float32)
        iterate = jnp.dot(
            iterate, 2.0 * identity - product, precision=lax.Precision.HIGHEST, preferred_element_type=jnp.float32
        )
    out[...] = iterate[:BLOCK, :BLOCK].astype(jnp.bfloat16)


def inverse(flag, shift, first, second, third):
    smem = pl.BlockSpec(memory_space=pltpu.SMEM)
    vmem = pl.BlockSpec(memory_space=pltpu.VMEM)
    return pl.pallas_call(
        inverse_kernel,
        in_specs=[smem, smem, vmem, vmem, vmem],
        out_specs=vmem,
        out_shape=jax.ShapeDtypeStruct((BLOCK, BLOCK), jnp.bfloat16),
        cost_estimate=pl.CostEstimate(flops=4_000_000_000, bytes_accessed=200_000, transcendentals=0),
        name="inverse",
    )(flag, shift, first, second, third)


def left_kernel(place, slots, weight, out):
    for slot in range(4):
        rows = pl.ds(pl.multiple_of((slot ^ place[0]) * BLOCK, BLOCK), BLOCK)
        out[rows, :] = jnp.dot(
            slots[slot], weight[rows, :], preferred_element_type=jnp.float32
        ).astype(jnp.bfloat16)


def left_product(place, slots, weight):
    return pl.pallas_call(
        left_kernel,
        in_specs=[pl.BlockSpec(memory_space=pltpu.SMEM)] + [pl.BlockSpec(memory_space=pltpu.VMEM)] * 2,
        out_specs=pl.BlockSpec(memory_space=pltpu.VMEM),
        out_shape=jax.ShapeDtypeStruct(weight.shape, jnp.bfloat16),
        cost_estimate=pl.CostEstimate(flops=2_000_000_000, bytes_accessed=5_000_000, transcendentals=0),
        name="left",
    )(place, slots, weight)


def natural_kernel(place, left, weight, *refs):
    slots, out, total = refs[:8], refs[8], refs[9]
    row = place[0]
    flip = lax.rem(row, 2) == 1
    total[...] = jnp.zeros_like(total)
    for pair in range(4):
        one, two = slots[2 * pair][...], slots[2 * pair + 1][...]
        even = jnp.where(flip, two, one)
        odd = jnp.where(flip, one, two)
        zero = jnp.zeros((BLOCK, BLOCK), jnp.bfloat16)
        both = jnp.concatenate(
            [jnp.concatenate([even, zero], axis=1), jnp.concatenate([zero, odd], axis=1)], axis=0
        )
        columns = pl.ds(pl.multiple_of((pair ^ (row // 2)) * 384, 384), 384)
        natural = jnp.dot(left[:, columns], both, preferred_element_type=jnp.float32)
        out[:, columns] = natural
        product = natural * weight[:, columns].astype(jnp.float32)
        folded = jnp.sum(product.reshape(96, 8, 384), axis=0)
        total[...] += folded[:, :128] + folded[:, 128:256] + folded[:, 256:]


def natural_product(place, left, weight, slots):
    vmem = pl.BlockSpec(memory_space=pltpu.VMEM)
    return pl.pallas_call(
        natural_kernel,
        in_specs=[pl.BlockSpec(memory_space=pltpu.SMEM)] + [vmem] * 10,
        out_specs=[vmem, vmem],
        out_shape=[
            jax.ShapeDtypeStruct(weight.shape, jnp.float32),
            jax.ShapeDtypeStruct((8, LANES), jnp.float32),
        ],
        cost_estimate=pl.CostEstimate(flops=3_000_000_000, bytes_accessed=10_000_000, transcendentals=0),
        name="natural",
    )(place, left, weight, *slots)


def exchange(slots, masks):
    got = [swap(slots[s], masks[s]) for s in range(1, 4)]
    return (slots[0] + got[1]) + (got[0] + got[2])


def on_device(tokens, grads, weight_grad):
    z = lax.axis_index("dp")
    x_low = lax.axis_index("row_0")
    y = lax.axis_index("row_1")
    x_high = lax.axis_index("col_0")
    core = lax.axis_index("col_1")
    x = 2 * x_high + x_low
    row = 4 * x_low + y
    ints = lambda *values: jnp.stack([jnp.asarray(v, jnp.int32) for v in values])

    def squares(array):
        wide = array.astype(jnp.float32)
        return jnp.sum(wide * wide)

    got_in = swap(lax.dynamic_slice_in_dim(tokens, (1 - core) * (D // 2), D // 2, 1), 1)
    got_out = []
    order = (2, 1, 3, 0)
    for sz in order:
        to = (z ^ sz) * 2
        halves = [
            lax.dynamic_slice_in_dim(grads, ((to + h) * 2 + 1 - core) * 1536, 1536, 1) for h in range(2)
        ]
        got_out.append(swap(jnp.concatenate(halves, axis=1), 1))
    traces = all_sum(jnp.stack([squares(tokens), squares(grads)]))
    trace_in, trace_out = traces[0] / TOKENS, traces[1] / TOKENS
    ratio = jnp.sqrt((trace_in / D + epsilon) / (trace_out / F + epsilon))
    damp_root = math.sqrt(damping)

    where = ints(*[core * 4 + (y ^ s) for s in range(4)], *[y ^ s for s in range(4)], x)
    pieces = in_blocks(where, tokens, got_in)
    a1 = exchange(pieces[:4], Y_MASKS)
    b1 = exchange(pieces[4:], X_MASKS)
    a2 = exchange([a1[s] for s in range(4)], X_MASKS)
    b2 = exchange([b1[s] for s in range(4)], Y_MASKS)
    both = jnp.concatenate([a2, b2], axis=0)
    both = exchange([both] * 4, Z_MASKS)
    own_in = inverse(
        ints(x_low),
        (ratio * damp_root).reshape(1),
        both[:64],
        jnp.concatenate([both[64:96], both[160:]], axis=0),
        both[96:160],
    )
    in_slots = jnp.stack([own_in] + [swap(own_in, mask) for mask in X_MASKS[1:]])
    in_slots = jnp.where(core == x_low, in_slots, swap(in_slots, 1))
    left = left_product(ints(x), in_slots, weight_grad)

    a1, b1, c0 = [None] * 4, [None] * 4, [None] * 4
    for sz, got in zip(order, got_out):
        to = [((z ^ sz) * 2 + (x ^ s) // 2, lax.rem(x ^ s, 2)) for s in range(4)]
        where = ints(*[(group * 2 + core) * 2 + low for group, low in to], *[x ^ s for s in range(4)], y)
        pieces = out_blocks(where, grads, got)
        a1[sz] = exchange(pieces[:4], X_MASKS)
        b1[sz] = exchange(pieces[4:8], Y_MASKS)
        c0[sz] = pieces[8]
    c1 = exchange(c0, Z_MASKS)
    a2 = exchange([jnp.stack([a1[sz][s] for sz in range(4)]) for s in range(4)], Y_MASKS)
    b2 = exchange(b1, Z_MASKS)
    c2 = exchange([c1[s] for s in range(4)], X_MASKS)
    a3 = exchange([a2[s] for s in range(4)], Z_MASKS)
    b3 = exchange([b2[s] for s in range(4)], X_MASKS)
    c3 = exchange([c2[s] for s in range(4)], Y_MASKS)
    own_out = inverse(ints(lax.rem(y, 2)), (damp_root / ratio).reshape(1), a3, b3, c3)
    out_slots = [own_out] + [swap(own_out, (s // 4) * 16 + (s % 4) * 4) for s in range(1, 8)]
    natural, partial = natural_product(ints(row), left, weight_grad, out_slots)
    alignment = jnp.sum(all_sum(partial))
    return (natural * jnp.sqrt(trust_radius * D * F / alignment)).astype(jnp.bfloat16)


def solution(mesh):
    finer = Mesh(mesh.devices.reshape(mesh.shape["dp"], 2, 4, 2, 2), ALL)
    placed = (P(ALL, None), P(ALL, None), P(ROW, DP_COL))
    return jax.shard_map(
        on_device, mesh=finer, in_specs=placed, out_specs=P(ROW, DP_COL), check_vma=False
    )
```

```python
import functools
import math

import jax
import jax.numpy as jnp
from jax import lax
from jax.experimental import pallas as pl
from jax.experimental.pallas import tpu as pltpu
from jax.sharding import Mesh
from jax.sharding import PartitionSpec as P

D = 6144
F = 24576
TOKENS = 32768
BLOCK = 192
STEPS = 3
ALL = ("dp", "row_0", "row_1", "col_0", "col_1")
ROW = ("row_0", "row_1")
DP_COL = ("dp", "col_0", "col_1")

epsilon = 1e-06
damping = 0.01
trust_radius = 0.05


X_BITS = (0, 16, 2, 18)
Y_BITS = (0, 4, 8, 12)
Z_BITS = (0, 32, 64, 96)
HALF = BLOCK // 3
LANES = 128
A_ROWS = 104
B_ROWS = 96
MIB = 1024 * 1024


def swap(array, near, far):
    return lax.ppermute(array, ALL, [(i, i ^ (far if i % 2 else near)) for i in range(128)])


def first(array, bits):
    return swap(array, bits[1], bits[3])


def second(array, bits):
    return swap(array, bits[3], bits[1])


def packed_pair(own, got, at):
    even = jnp.zeros((BLOCK, 256), jnp.float32)
    odd = jnp.zeros((BLOCK, 256), jnp.float32)
    for ref in (own, got):
        part = ref[:, at : at + 384]
        turned = part.T
        even += jnp.dot(turned[:BLOCK], part[:, :256], preferred_element_type=jnp.float32)
        odd += jnp.dot(turned[BLOCK:], part[:, 128:], preferred_element_type=jnp.float32)
    low = lax.broadcasted_iota(jnp.int32, (HALF, LANES), 1) < HALF
    e = [[even[HALF * i : HALF * (i + 1), LANES * j : LANES * (j + 1)] for j in range(2)] for i in range(3)]
    o = [[odd[HALF * i : HALF * (i + 1), LANES * j : LANES * (j + 1)] for j in range(2)] for i in range(3)]
    evens = (e[0][0], jnp.where(low, e[0][1], e[1][0]), jnp.where(low, e[2][1], e[2][0]))
    odds = (jnp.where(low, o[0][1], o[0][0]), jnp.where(low, o[1][1], o[0][1]), o[2][1])
    return evens, odds


def out_kernel(where, own, got, a_send, a_keep, b_send, b_keep, c_out):
    step = pl.program_id(0)
    v_z = step // 4
    x_slot = lax.rem(step, 4)
    u_x, v_x = x_slot // 2, lax.rem(x_slot, 2)
    for pair in range(2):
        pieces = packed_pair(own, got, pair * 384)
        for parity in range(2):
            piece = pieces[parity]
            u_y = where[16 + 2 * pair + parity]
            v_y = where[20 + 2 * pair + parity]

            @pl.when(u_x == 1)
            def _():
                a_send[v_z, v_x, 2 * u_y + v_y] = piece[0]

            @pl.when(u_x == 0)
            def _():
                a_keep[v_z, v_x, 2 * u_y + v_y] = piece[0]

            @pl.when(u_y == 1)
            def _():
                b_send[v_y, v_z, x_slot] = piece[1]

            @pl.when(u_y == 0)
            def _():
                b_keep[v_y, v_z, x_slot] = piece[1]

            c_out[v_z, x_slot, 2 * u_y + v_y] = piece[2]


def out_blocks(where, own, got):
    shapes = [(2, 2, 4, HALF, LANES)] * 4 + [(2, 4, 4, HALF, LANES)]
    return pl.pallas_call(
        out_kernel,
        grid_spec=pltpu.PrefetchScalarGridSpec(
            num_scalar_prefetch=1,
            grid=(8,),
            in_specs=[
                pl.BlockSpec((256, 768), lambda i, w: (0, w[i])),
                pl.BlockSpec((256, 768), lambda i, w: (0, w[8 + i])),
            ],
            out_specs=[pl.BlockSpec(s, lambda i, w: (0, 0, 0, 0, 0)) for s in shapes],
        ),
        out_shape=[jax.ShapeDtypeStruct(s, jnp.float32) for s in shapes],
        cost_estimate=pl.CostEstimate(flops=10_000_000_000, bytes_accessed=10_000_000, transcendentals=0),
        compiler_params=pltpu.CompilerParams(vmem_limit_bytes=24 * MIB),
        name="cov_out",
    )(where, own, got)


def in_kernel(where, own, got, trace_own, trace_got, a_send, a_keep, b_send, b_keep):
    y_slot = pl.program_id(0)
    u_y, v_y = y_slot // 2, lax.rem(y_slot, 2)
    trace = trace_own[...] + trace_got[...]
    for pair in range(2):
        pieces = packed_pair(own, got, pair * 384)
        for parity in range(2):
            piece = pieces[parity]
            u_x = where[8 + 2 * pair + parity]
            v_x = where[12 + 2 * pair + parity]

            def store_a(ref):
                slot = 2 * u_x + v_x
                ref[v_y, slot, :64] = piece[0]
                ref[v_y, slot, 64:96] = piece[1][:32]
                ref[v_y, slot, 96:] = trace

            def store_b(ref):
                ref[v_x, y_slot, :64] = piece[2]
                ref[v_x, y_slot, 64:] = piece[1][32:]

            pl.when(u_y == 1)(functools.partial(store_a, a_send))
            pl.when(u_y == 0)(functools.partial(store_a, a_keep))
            pl.when(u_x == 1)(functools.partial(store_b, b_send))
            pl.when(u_x == 0)(functools.partial(store_b, b_keep))


def in_blocks(where, own, got, trace_own, trace_got):
    shapes = [(2, 4, A_ROWS, LANES)] * 2 + [(2, 4, B_ROWS, LANES)] * 2
    return pl.pallas_call(
        in_kernel,
        grid_spec=pltpu.PrefetchScalarGridSpec(
            num_scalar_prefetch=1,
            grid=(4,),
            in_specs=[
                pl.BlockSpec((256, 768), lambda i, w: (0, w[i])),
                pl.BlockSpec((256, 768), lambda i, w: (0, w[4 + i])),
                pl.BlockSpec((8, LANES), lambda i, w: (0, 0)),
                pl.BlockSpec((8, LANES), lambda i, w: (0, 0)),
            ],
            out_specs=[pl.BlockSpec(s, lambda i, w: (0, 0, 0, 0)) for s in shapes],
        ),
        out_shape=[jax.ShapeDtypeStruct(s, jnp.float32) for s in shapes],
        cost_estimate=pl.CostEstimate(flops=5_000_000_000, bytes_accessed=5_000_000, transcendentals=0),
        compiler_params=pltpu.CompilerParams(vmem_limit_bytes=16 * MIB),
        name="cov_in",
    )(where, own, got, trace_own, trace_got)


def squares_kernel(tokens, grads, out):
    @pl.when(pl.program_id(0) == 0)
    def _():
        out[...] = jnp.zeros_like(out)

    for ref, row in ((tokens, 0), (grads, 4)):
        parts = []
        for at in range(0, ref.shape[1], 256):
            wide = ref[:, at : at + 256].astype(jnp.float32)
            total = jnp.sum((wide * wide).reshape(32, 8, 256), axis=0)
            parts.append(total[:, :128] + total[:, 128:])
        total = functools.reduce(jnp.add, parts)
        out[row : row + 4, :] += total[:4] + total[4:]


def squares(tokens, grads):
    return pl.pallas_call(
        squares_kernel,
        grid=(8,),
        in_specs=[
            pl.BlockSpec((256, D // 8), lambda i: (0, i)),
            pl.BlockSpec((256, F // 8), lambda i: (0, i)),
        ],
        out_specs=pl.BlockSpec((8, LANES), lambda i: (0, 0)),
        out_shape=jax.ShapeDtypeStruct((8, LANES), jnp.float32),
        cost_estimate=pl.CostEstimate(flops=3_000_000_000, bytes_accessed=15_000_000, transcendentals=0),
        compiler_params=pltpu.CompilerParams(vmem_limit_bytes=16 * MIB),
        name="squares",
    )(tokens, grads)


def newton(pieces, trace, swapped, inward):
    total_in = jnp.sum(trace[:4], axis=(0, 1), keepdims=True) * (1.0 / TOKENS)
    total_out = jnp.sum(trace[4:], axis=(0, 1), keepdims=True) * (1.0 / TOKENS)
    ratio = jnp.sqrt((total_in / D + epsilon) / (total_out / F + epsilon))
    damp_root = math.sqrt(damping)
    shift = ratio * damp_root if inward else damp_root / ratio
    c = [jnp.where(swapped, pltpu.roll(value, HALF, 1), value) for value in pieces]
    t = [jnp.concatenate([value, value], axis=0).T for value in c]
    low = lax.broadcasted_iota(jnp.int32, (HALF, LANES), 1) < HALF
    zero = jnp.zeros((HALF, LANES), jnp.float32)
    rows = [
        [c[0], jnp.where(low, c[1], zero)],
        [jnp.where(low, t[0][HALF:], c[1]), jnp.where(low, t[2][HALF:], zero)],
        [jnp.where(low, t[1][:HALF], c[2]), jnp.where(low, c[2], zero)],
        [zero, zero],
    ]
    blocks = jnp.concatenate([jnp.concatenate(pair, axis=1) for pair in rows], axis=0)
    i = lax.broadcasted_iota(jnp.int32, (256, 256), 0)
    j = lax.broadcasted_iota(jnp.int32, (256, 256), 1)
    identity = jnp.where((i == j) & (i < BLOCK), 1.0, 0.0).astype(jnp.float32)
    matrix = blocks * (1.0 / TOKENS) + shift * identity
    total = jnp.sum(matrix * matrix, axis=(0, 1), keepdims=True)
    iterate = identity / jnp.sqrt(total)
    for sweep in range(STEPS):
        product = jnp.dot(matrix, iterate, precision=lax.Precision.HIGHEST, preferred_element_type=jnp.float32)
        iterate = jnp.dot(
            iterate, 2.0 * identity - product, precision=lax.Precision.HIGHEST, preferred_element_type=jnp.float32
        )
    return iterate[:BLOCK, :BLOCK].astype(jnp.bfloat16)


def inverse_in_kernel(flag, one, two, out, trace_out):
    both = one[...] + two[...]
    trace = both[96:104]
    trace_out[...] = trace
    middle = jnp.concatenate([both[64:96], both[168:200]], axis=0)
    out[...] = newton([both[:64], middle, both[104:168]], trace, flag[0] == 1, True)


def inverse_out_kernel(flag, trace, a0, a1, b0, b1, c0, c1, out):
    pieces = [a0[...] + a1[...], b0[...] + b1[...], c0[...] + c1[...]]
    out[...] = newton(pieces, trace[...], flag[0] == 1, False)


def inverse(kernel, flag, args, with_trace):
    vmem = pl.BlockSpec(memory_space=pltpu.VMEM)
    shape = jax.ShapeDtypeStruct((BLOCK, BLOCK), jnp.bfloat16)
    return pl.pallas_call(
        kernel,
        in_specs=[pl.BlockSpec(memory_space=pltpu.SMEM)] + [vmem] * len(args),
        out_specs=[vmem, vmem] if with_trace else vmem,
        out_shape=[shape, jax.ShapeDtypeStruct((8, LANES), jnp.float32)] if with_trace else shape,
        cost_estimate=pl.CostEstimate(flops=4_000_000_000, bytes_accessed=200_000, transcendentals=0),
        name="inverse",
    )(flag, *args)


def left_kernel(place, slots, weight, out):
    for slot in range(4):
        rows = pl.ds(pl.multiple_of(place[slot] * BLOCK, BLOCK), BLOCK)
        out[rows, :] = jnp.dot(
            slots[slot], weight[rows, :], preferred_element_type=jnp.float32
        ).astype(jnp.bfloat16)


def left_product(place, slots, weight):
    return pl.pallas_call(
        left_kernel,
        in_specs=[pl.BlockSpec(memory_space=pltpu.SMEM)] + [pl.BlockSpec(memory_space=pltpu.VMEM)] * 2,
        out_specs=pl.BlockSpec(memory_space=pltpu.VMEM),
        out_shape=jax.ShapeDtypeStruct(weight.shape, jnp.bfloat16),
        cost_estimate=pl.CostEstimate(flops=2_000_000_000, bytes_accessed=5_000_000, transcendentals=0),
        name="left",
    )(place, slots, weight)


def natural_kernel(place, left, weight, mine, theirs, out, total):
    total[...] = jnp.zeros_like(total)
    zero = jnp.zeros((BLOCK, BLOCK), jnp.bfloat16)

    def inverse_of(block):
        slot = place[block]
        return jnp.where(place[8 + block] == 1, theirs[slot], mine[slot])

    for pair in range(4):
        both = jnp.concatenate(
            [
                jnp.concatenate([inverse_of(2 * pair), zero], axis=1),
                jnp.concatenate([zero, inverse_of(2 * pair + 1)], axis=1),
            ],
            axis=0,
        )
        columns = slice(384 * pair, 384 * (pair + 1))
        natural = jnp.dot(left[:, columns], both, preferred_element_type=jnp.float32)
        out[:, columns] = natural
        product = natural * weight[:, columns].astype(jnp.float32)
        folded = jnp.sum(product.reshape(96, 8, 384), axis=0)
        total[...] += folded[:, :128] + folded[:, 128:256] + folded[:, 256:]


def natural_product(place, left, weight, mine, theirs):
    vmem = pl.BlockSpec(memory_space=pltpu.VMEM)
    return pl.pallas_call(
        natural_kernel,
        in_specs=[pl.BlockSpec(memory_space=pltpu.SMEM)] + [vmem] * 4,
        out_specs=[vmem, vmem],
        out_shape=[
            jax.ShapeDtypeStruct(weight.shape, jnp.float32),
            jax.ShapeDtypeStruct((8, LANES), jnp.float32),
        ],
        cost_estimate=pl.CostEstimate(flops=3_000_000_000, bytes_accessed=10_000_000, transcendentals=0),
        name="natural",
    )(place, left, weight, mine, theirs)


def ints(*values):
    return jnp.stack([jnp.asarray(v, jnp.int32) for v in values])


def on_device(tokens, grads, weight_grad):
    z = lax.axis_index("dp")
    x_low = lax.axis_index("row_0")
    y = lax.axis_index("row_1")
    x_high = lax.axis_index("col_0")
    core = lax.axis_index("col_1")
    x = 2 * x_high + x_low

    def near(c):
        return 1 + 2 * c

    def slots_of(c, at):
        return at, at ^ (4 - near(c)), at ^ near(c), at ^ 2

    def bits_of(c, mask):
        u = (mask == 2) | (mask == near(c))
        v = (mask == 2) | (mask == 4 - near(c))
        return u.astype(jnp.int32), v.astype(jnp.int32)

    other = 1 - core
    got_in = swap(lax.dynamic_slice_in_dim(tokens, other * (D // 2), D // 2, 1), 1, 1)
    z_other = slots_of(other, z)
    got_out = {}
    for u_z in (1, 0):
        quarters = [
            lax.dynamic_slice_in_dim(grads, ((z_other[2 * u_z + v] * 2 + h) * 2 + other) * 1536, 1536, 1)
            for v in range(2)
            for h in range(2)
        ]
        got_out[u_z] = swap(jnp.concatenate(quarters, axis=1), 1, 1)
    trace = squares(tokens, grads)

    x_slots, y_slots, z_slots = slots_of(core, x), slots_of(core, y), slots_of(core, z)
    x_bits = [bits_of(core, x ^ q) for q in range(4)]
    y_bits = [bits_of(core, y ^ q) for q in range(4)]

    where = ints(
        *[core * 4 + at for at in y_slots], *y_slots, *[b[0] for b in x_bits], *[b[1] for b in x_bits]
    )
    a_send, a_keep, b_send, b_keep = in_blocks(where, tokens, got_in, trace, swap(trace, 1, 1))
    a = a_keep + first(a_send, Y_BITS)
    b = b_keep + first(b_send, X_BITS)
    a = a[0] + second(a[1], Y_BITS)
    b = b[0] + second(b[1], X_BITS)
    a = a[:2] + first(a[2:], X_BITS)
    b = b[:2] + first(b[2:], Y_BITS)
    a = a[0] + second(a[1], X_BITS)
    b = b[0] + second(b[1], Y_BITS)
    both = jnp.concatenate([a, b], axis=0)
    both = both + first(both, Z_BITS)
    own, trace = inverse(inverse_in_kernel, ints(x_low), [both, second(both, Z_BITS)], True)
    slots = jnp.stack([own, first(own, X_BITS)])
    slots = jnp.concatenate([slots, second(slots, X_BITS)], axis=0)
    slots = jnp.where(core == x_low, slots, swap(slots, 1, 1))
    place = slots_of(x_low, x)
    left = left_product(ints(place[0], place[2], place[1], place[3]), slots, weight_grad)

    where = {
        u_z: ints(
            *[((z_slots[2 * u_z + v] * 2 + at // 2) * 2 + core) * 2 + lax.rem(at, 2) for v in range(2) for at in x_slots],
            *[4 * v + at for v in range(2) for at in x_slots],
            *[b[0] for b in y_bits],
            *[b[1] for b in y_bits],
        )
        for u_z in range(2)
    }
    a, b, c = {}, {}, {}
    for u_z in (1, 0):
        a_send, a_keep, b_send, b_keep, c[u_z] = out_blocks(where[u_z], grads, got_out[u_z])
        a[u_z] = a_keep + first(a_send, X_BITS)
        b[u_z] = b_keep + first(b_send, Y_BITS)
    c = c[0] + first(c[1], Z_BITS)
    a = [jnp.stack([a[0][:, v], a[1][:, v]]) for v in range(2)]
    b = [jnp.stack([b[0][v], b[1][v]]) for v in range(2)]
    a = a[0] + second(a[1], X_BITS)
    b = b[0] + second(b[1], Y_BITS)
    c = c[0] + second(c[1], Z_BITS)
    a = a[:, :, :2] + first(a[:, :, 2:], Y_BITS)
    b = b[0] + first(b[1], Z_BITS)
    c = c[:2] + first(c[2:], X_BITS)
    a = a[:, :, 0] + second(a[:, :, 1], Y_BITS)
    b = b[0] + second(b[1], Z_BITS)
    c = c[0] + second(c[1], X_BITS)
    a = a[0] + first(a[1], Z_BITS)
    b = b[:2] + first(b[2:], X_BITS)
    c = c[:2] + first(c[2:], Y_BITS)
    pieces = [a[0], second(a[1], Z_BITS), b[0], second(b[1], X_BITS), c[0], second(c[1], Y_BITS)]
    own = inverse(inverse_out_kernel, ints(lax.rem(y, 2)), [trace] + pieces, False)
    mine = jnp.stack([own, swap(own, 16, 16)])
    mine = jnp.concatenate([mine, first(mine, Y_BITS)], axis=0)
    theirs = second(mine, Y_BITS)
    place = ints(
        *[2 * y_bits[r % 4][0] + (x_low ^ (r // 4)) for r in range(8)], *[y_bits[r % 4][1] for r in range(8)]
    )
    natural, total = natural_product(place, left, weight_grad, mine, theirs)
    total = total + swap(total, 1, 1)
    for bits in (X_BITS, Y_BITS, Z_BITS):
        total = total + first(total, bits)
        total = total + second(total, bits)
    alignment = jnp.sum(total)
    return (natural * jnp.sqrt(trust_radius * D * F / alignment)).astype(jnp.bfloat16)


def solution(mesh):
    finer = Mesh(mesh.devices.reshape(mesh.shape["dp"], 2, 4, 2, 2), ALL)
    placed = (P(ALL, None), P(ALL, None), P(ROW, DP_COL))
    return jax.shard_map(
        on_device, mesh=finer, in_specs=placed, out_specs=P(ROW, DP_COL), check_vma=False
    )
```

```python
import functools
import math

import jax
import jax.numpy as jnp
from jax import lax
from jax.experimental import pallas as pl
from jax.experimental.pallas import tpu as pltpu
from jax.sharding import Mesh
from jax.sharding import PartitionSpec as P

D = 6144
F = 24576
TOKENS = 32768
BLOCK = 192
STEPS = 3
ALL = ("dp", "row_0", "row_1", "col_0", "col_1")
ROW = ("row_0", "row_1")
DP_COL = ("dp", "col_0", "col_1")

epsilon = 1e-06
damping = 0.01
trust_radius = 0.05


X_BITS = (0, 16, 2, 18)
Y_BITS = (0, 4, 8, 12)
Z_BITS = (0, 32, 64, 96)
HALF = BLOCK // 3
LANES = 128
IN_ROWS = BLOCK + 8
MIB = 1024 * 1024


def swap(array, near, far):
    return lax.ppermute(array, ALL, [(i, i ^ (far if i % 2 else near)) for i in range(128)])


def first(array, bits):
    return swap(array, bits[1], bits[3])


def second(array, bits):
    return swap(array, bits[3], bits[1])


def packed_pair(own, got, at):
    even = jnp.zeros((BLOCK, 256), jnp.float32)
    odd = jnp.zeros((BLOCK, 256), jnp.float32)
    for ref in (own, got):
        part = ref[:, at : at + 384]
        turned = part.T
        even += jnp.dot(turned[:BLOCK], part[:, :256], preferred_element_type=jnp.float32)
        odd += jnp.dot(turned[BLOCK:], part[:, 128:], preferred_element_type=jnp.float32)
    low = lax.broadcasted_iota(jnp.int32, (HALF, LANES), 1) < HALF
    e = [[even[HALF * i : HALF * (i + 1), LANES * j : LANES * (j + 1)] for j in range(2)] for i in range(3)]
    o = [[odd[HALF * i : HALF * (i + 1), LANES * j : LANES * (j + 1)] for j in range(2)] for i in range(3)]
    evens = (e[0][0], jnp.where(low, e[0][1], e[1][0]), jnp.where(low, e[2][1], e[2][0]))
    odds = (jnp.where(low, o[0][1], o[0][0]), jnp.where(low, o[1][1], o[0][1]), o[2][1])
    return evens, odds


def out_kernel(where, own, got, a_send, a_keep, b_send, b_keep, c_out):
    step = pl.program_id(0)
    v_z = step // 4
    x_slot = lax.rem(step, 4)
    u_x, v_x = x_slot // 2, lax.rem(x_slot, 2)
    for pair in range(2):
        pieces = packed_pair(own, got, pair * 384)
        for parity in range(2):
            piece = pieces[parity]
            u_y = where[16 + 2 * pair + parity]
            v_y = where[20 + 2 * pair + parity]

            @pl.when(u_x == 1)
            def _():
                a_send[v_z, v_x, 2 * u_y + v_y] = piece[0]

            @pl.when(u_x == 0)
            def _():
                a_keep[v_z, v_x, 2 * u_y + v_y] = piece[0]

            @pl.when(u_y == 1)
            def _():
                b_send[v_z, x_slot, v_y] = piece[1]

            @pl.when(u_y == 0)
            def _():
                b_keep[v_z, x_slot, v_y] = piece[1]

            c_out[v_z, x_slot, 2 * u_y + v_y] = piece[2]


def out_blocks(where, own, got):
    shapes = [(2, 2, 4, HALF, LANES)] * 2 + [(2, 4, 2, HALF, LANES)] * 2 + [(2, 4, 4, HALF, LANES)]
    return pl.pallas_call(
        out_kernel,
        grid_spec=pltpu.PrefetchScalarGridSpec(
            num_scalar_prefetch=1,
            grid=(8,),
            in_specs=[
                pl.BlockSpec((256, 768), lambda i, w: (0, w[i])),
                pl.BlockSpec((256, 768), lambda i, w: (0, w[8 + i])),
            ],
            out_specs=[pl.BlockSpec(s, lambda i, w: (0, 0, 0, 0, 0)) for s in shapes],
        ),
        out_shape=[jax.ShapeDtypeStruct(s, jnp.float32) for s in shapes],
        cost_estimate=pl.CostEstimate(flops=10_000_000_000, bytes_accessed=10_000_000, transcendentals=0),
        compiler_params=pltpu.CompilerParams(vmem_limit_bytes=48 * MIB),
        name="cov_out",
    )(where, own, got)


def in_kernel(where, own, got, trace_own, trace_got, send, keep):
    y_slot = pl.program_id(0)
    u_y, v_y = y_slot // 2, lax.rem(y_slot, 2)
    trace = trace_own[...] + trace_got[...]
    for pair in range(2):
        pieces = packed_pair(own, got, pair * 384)
        for parity in range(2):
            piece = pieces[parity]
            slot = where[8 + 2 * pair + parity]

            def store(ref):
                for i in range(3):
                    ref[v_y, slot, HALF * i : HALF * (i + 1)] = piece[i]
                ref[v_y, slot, BLOCK:] = trace

            pl.when(u_y == 1)(functools.partial(store, send))
            pl.when(u_y == 0)(functools.partial(store, keep))


def in_blocks(where, own, got, trace_own, trace_got):
    shape = (2, 4, IN_ROWS, LANES)
    return pl.pallas_call(
        in_kernel,
        grid_spec=pltpu.PrefetchScalarGridSpec(
            num_scalar_prefetch=1,
            grid=(4,),
            in_specs=[
                pl.BlockSpec((256, 768), lambda i, w: (0, w[i])),
                pl.BlockSpec((256, 768), lambda i, w: (0, w[4 + i])),
                pl.BlockSpec((8, LANES), lambda i, w: (0, 0)),
                pl.BlockSpec((8, LANES), lambda i, w: (0, 0)),
            ],
            out_specs=[pl.BlockSpec(shape, lambda i, w: (0, 0, 0, 0))] * 2,
        ),
        out_shape=[jax.ShapeDtypeStruct(shape, jnp.float32)] * 2,
        cost_estimate=pl.CostEstimate(flops=5_000_000_000, bytes_accessed=5_000_000, transcendentals=0),
        compiler_params=pltpu.CompilerParams(vmem_limit_bytes=48 * MIB),
        name="cov_in",
    )(where, own, got, trace_own, trace_got)


def squares_of(ref):
    parts = []
    for at in range(0, ref.shape[1], 256):
        wide = ref[:, at : at + 256].astype(jnp.float32)
        total = jnp.sum((wide * wide).reshape(32, 8, 256), axis=0)
        parts.append(total[:, :128] + total[:, 128:])
    total = functools.reduce(jnp.add, parts)
    return total[:4] + total[4:]


def tokens_kernel(where, tokens, out, total):
    @pl.when(pl.program_id(0) == 0)
    def _():
        out[...] = tokens[...]
        total[...] = jnp.zeros_like(total)

    total[:4] += squares_of(tokens)


def tokens_share(where, tokens):
    return pl.pallas_call(
        tokens_kernel,
        grid_spec=pltpu.PrefetchScalarGridSpec(
            num_scalar_prefetch=1,
            grid=(2,),
            in_specs=[pl.BlockSpec((256, D // 2), lambda i, w: (0, w[i]))],
            out_specs=[
                pl.BlockSpec((256, D // 2), lambda i, w: (0, 0)),
                pl.BlockSpec((8, LANES), lambda i, w: (0, 0)),
            ],
        ),
        out_shape=[
            jax.ShapeDtypeStruct((256, D // 2), jnp.bfloat16),
            jax.ShapeDtypeStruct((8, LANES), jnp.float32),
        ],
        cost_estimate=pl.CostEstimate(flops=500_000_000, bytes_accessed=5_000_000, transcendentals=0),
        compiler_params=pltpu.CompilerParams(vmem_limit_bytes=48 * MIB),
        name="tokens_share",
    )(where, tokens)


def grads_kernel(where, grads, before, one, two, total):
    step = pl.program_id(0)

    @pl.when(step == 0)
    def _():
        total[...] = before[...]

    @pl.when(step < 4)
    def _():
        one[...] = grads[...]

    @pl.when((step >= 4) & (step < 8))
    def _():
        two[...] = grads[...]

    total[4:] += squares_of(grads)


def grads_share(where, grads, before):
    return pl.pallas_call(
        grads_kernel,
        grid_spec=pltpu.PrefetchScalarGridSpec(
            num_scalar_prefetch=1,
            grid=(16,),
            in_specs=[
                pl.BlockSpec((256, 1536), lambda i, w: (0, w[i])),
                pl.BlockSpec((8, LANES), lambda i, w: (0, 0)),
            ],
            out_specs=[
                pl.BlockSpec((256, 1536), lambda i, w: (0, jnp.minimum(i, 3))),
                pl.BlockSpec((256, 1536), lambda i, w: (0, jnp.clip(i - 4, 0, 3))),
                pl.BlockSpec((8, LANES), lambda i, w: (0, 0)),
            ],
        ),
        out_shape=[jax.ShapeDtypeStruct((256, 6144), jnp.bfloat16)] * 2
        + [jax.ShapeDtypeStruct((8, LANES), jnp.float32)],
        cost_estimate=pl.CostEstimate(flops=2_000_000_000, bytes_accessed=20_000_000, transcendentals=0),
        compiler_params=pltpu.CompilerParams(vmem_limit_bytes=48 * MIB),
        name="grads_share",
    )(where, grads, before)


def newton(pieces, trace, swapped, inward):
    total_in = jnp.sum(trace[:4], axis=(0, 1), keepdims=True) * (1.0 / TOKENS)
    total_out = jnp.sum(trace[4:], axis=(0, 1), keepdims=True) * (1.0 / TOKENS)
    ratio = jnp.sqrt((total_in / D + epsilon) / (total_out / F + epsilon))
    damp_root = math.sqrt(damping)
    shift = ratio * damp_root if inward else damp_root / ratio
    c = [jnp.where(swapped, pltpu.roll(value, HALF, 1), value) for value in pieces]
    t = [jnp.concatenate([value, value], axis=0).T for value in c]
    low = lax.broadcasted_iota(jnp.int32, (HALF, LANES), 1) < HALF
    zero = jnp.zeros((HALF, LANES), jnp.float32)
    rows = [
        [c[0], jnp.where(low, c[1], zero)],
        [jnp.where(low, t[0][HALF:], c[1]), jnp.where(low, t[2][HALF:], zero)],
        [jnp.where(low, t[1][:HALF], c[2]), jnp.where(low, c[2], zero)],
        [zero, zero],
    ]
    blocks = jnp.concatenate([jnp.concatenate(pair, axis=1) for pair in rows], axis=0)
    i = lax.broadcasted_iota(jnp.int32, (256, 256), 0)
    j = lax.broadcasted_iota(jnp.int32, (256, 256), 1)
    identity = jnp.where((i == j) & (i < BLOCK), 1.0, 0.0).astype(jnp.float32)
    matrix = blocks * (1.0 / TOKENS) + shift * identity
    total = jnp.sum(matrix * matrix, axis=(0, 1), keepdims=True)
    iterate = identity / jnp.sqrt(total)
    for sweep in range(STEPS):
        product = jnp.dot(matrix, iterate, precision=lax.Precision.HIGHEST, preferred_element_type=jnp.float32)
        iterate = jnp.dot(
            iterate, 2.0 * identity - product, precision=lax.Precision.HIGHEST, preferred_element_type=jnp.float32
        )
    return iterate[:BLOCK, :BLOCK].astype(jnp.bfloat16)


def inverse_in_kernel(flag, one, two, out, trace_out):
    both = one[...] + two[...]
    trace = both[BLOCK:]
    trace_out[...] = trace
    pieces = [both[HALF * i : HALF * (i + 1)] for i in range(3)]
    out[...] = newton(pieces, trace, flag[0] == 1, True)


def inverse_out_kernel(flag, trace, slots, out):
    both = (slots[0] + slots[1] + (slots[2] + slots[3])) + (slots[4] + slots[5] + (slots[6] + slots[7]))
    pieces = [both[HALF * i : HALF * (i + 1)] for i in range(3)]
    out[...] = newton(pieces, trace[...], flag[0] == 1, False)


def inverse(kernel, flag, args, with_trace):
    vmem = pl.BlockSpec(memory_space=pltpu.VMEM)
    shape = jax.ShapeDtypeStruct((BLOCK, BLOCK), jnp.bfloat16)
    return pl.pallas_call(
        kernel,
        in_specs=[pl.BlockSpec(memory_space=pltpu.SMEM)] + [vmem] * len(args),
        out_specs=[vmem, vmem] if with_trace else vmem,
        out_shape=[shape, jax.ShapeDtypeStruct((8, LANES), jnp.float32)] if with_trace else shape,
        cost_estimate=pl.CostEstimate(flops=4_000_000_000, bytes_accessed=200_000, transcendentals=0),
        name="inverse",
    )(flag, *args)


def left_kernel(place, slots, weight, out):
    for slot in range(4):
        rows = pl.ds(pl.multiple_of(place[slot] * BLOCK, BLOCK), BLOCK)
        out[rows, :] = jnp.dot(
            slots[slot], weight[rows, :], preferred_element_type=jnp.float32
        ).astype(jnp.bfloat16)


def left_product(place, slots, weight):
    return pl.pallas_call(
        left_kernel,
        in_specs=[pl.BlockSpec(memory_space=pltpu.SMEM)] + [pl.BlockSpec(memory_space=pltpu.VMEM)] * 2,
        out_specs=pl.BlockSpec(memory_space=pltpu.VMEM),
        out_shape=jax.ShapeDtypeStruct(weight.shape, jnp.bfloat16),
        cost_estimate=pl.CostEstimate(flops=2_000_000_000, bytes_accessed=5_000_000, transcendentals=0),
        name="left",
    )(place, slots, weight)


def natural_kernel(left, weight, inverses, out, total):
    zero = jnp.zeros((BLOCK, BLOCK), jnp.bfloat16)
    sums = jnp.zeros((8, LANES), jnp.float32)
    for pair in range(4):
        both = jnp.concatenate(
            [
                jnp.concatenate([inverses[2 * pair], zero], axis=1),
                jnp.concatenate([zero, inverses[2 * pair + 1]], axis=1),
            ],
            axis=0,
        )
        columns = slice(384 * pair, 384 * (pair + 1))
        natural = jnp.dot(left[:, columns], both, preferred_element_type=jnp.float32)
        out[:, columns] = natural
        product = natural * weight[:, columns].astype(jnp.float32)
        folded = jnp.sum(product.reshape(96, 8, 384), axis=0)
        sums += folded[:, :128] + folded[:, 128:256] + folded[:, 256:]
    total[...] = jnp.broadcast_to(jnp.sum(sums, axis=0, keepdims=True), (128, LANES))


def natural_product(left, weight, inverses):
    vmem = pl.BlockSpec(memory_space=pltpu.VMEM)
    return pl.pallas_call(
        natural_kernel,
        in_specs=[vmem] * 3,
        out_specs=[vmem, vmem],
        out_shape=[
            jax.ShapeDtypeStruct(weight.shape, jnp.float32),
            jax.ShapeDtypeStruct((128, LANES), jnp.float32),
        ],
        cost_estimate=pl.CostEstimate(flops=3_000_000_000, bytes_accessed=10_000_000, transcendentals=0),
        name="natural",
    )(left, weight, inverses)


def ints(*values):
    return jnp.stack([jnp.asarray(v, jnp.int32) for v in values])


def cubes():
    groups = {}
    for i in range(128):
        z, x_low, y, x_high, core = i // 32, i // 16 % 2, i // 4 % 4, i // 2 % 2, i % 2
        x = 2 * x_high + x_low
        top = [at // 2 if core == 0 else at % 2 for at in (z, x, y)]
        rest = tuple(at % 2 ^ at // 2 if core == 0 else at // 2 for at in (z, x, y))
        groups.setdefault((core, rest), {})[tuple(top)] = i
    return [[members[k] for k in sorted(members)] for members in groups.values()]


def on_device(tokens, grads, weight_grad):
    z = lax.axis_index("dp")
    x_low = lax.axis_index("row_0")
    y = lax.axis_index("row_1")
    x_high = lax.axis_index("col_0")
    core = lax.axis_index("col_1")
    x = 2 * x_high + x_low
    other = 1 - core

    def near(c):
        return 1 + 2 * c

    def side(c, at):
        return jnp.where(c == 0, at // 2, lax.rem(at, 2))

    def slot_of(c, at, to):
        mask = at ^ to
        u = (mask == 2) | (mask == near(c))
        return 2 * u.astype(jnp.int32) + side(c, to)

    def slots_of(c, at):
        places = []
        for u in range(2):
            one = at ^ (u * near(c))
            two = one ^ (4 - near(c))
            low = side(c, one) == 0
            places += [jnp.where(low, one, two), jnp.where(low, two, one)]
        return places

    half, trace = tokens_share(ints(other, core), tokens)
    got_in = swap(half, 1, 1)
    z_other = slots_of(other, z)
    chunks = [(at * 2 + h) * 2 for at in z_other[2:] + z_other[:2] for h in range(2)]
    one, two, trace = grads_share(ints(*[at + other for at in chunks], *[at + core for at in chunks]), grads, trace)
    got_out = {1: swap(one, 1, 1), 0: swap(two, 1, 1)}

    x_slots, y_slots, z_slots = slots_of(core, x), slots_of(core, y), slots_of(core, z)
    slot_y = [slot_of(core, y, at) for at in range(4)]

    where = ints(*[core * 4 + at for at in y_slots], *y_slots, *[slot_of(core, x, at) for at in range(4)])
    send, keep = in_blocks(where, tokens, got_in, trace, swap(trace, 1, 1))
    y_side, x_side = side(core, y), side(core, x)

    def pick(array, at):
        return lax.dynamic_index_in_dim(array, at, 0, keepdims=False)

    both = keep + first(send, Y_BITS)
    both = pick(both, y_side) + second(pick(both, 1 - y_side), Y_BITS)
    both = both[:2] + first(both[2:], X_BITS)
    both = pick(both, x_side) + second(pick(both, 1 - x_side), X_BITS)
    both = both + first(both, Z_BITS)
    own, trace = inverse(inverse_in_kernel, ints(x_low), [both, second(both, Z_BITS)], True)
    slots = jnp.stack([own, first(own, X_BITS)])
    slots = jnp.concatenate([slots, second(slots, X_BITS)], axis=0)
    slots = jnp.where(core == x_low, slots, swap(slots, 1, 1))
    g = near(x_low)
    left = left_product(ints(x, x ^ g, x ^ (4 - g), x ^ 2), slots, weight_grad)

    where = {
        u_z: ints(
            *[
                ((at_z * 2 + at // 2) * 2 + core) * 2 + lax.rem(at, 2)
                for at_z in z_slots[2 * u_z : 2 * u_z + 2]
                for at in x_slots
            ],
            *[4 * v + at for v in range(2) for at in x_slots],
            *[s // 2 for s in slot_y],
            *[lax.rem(s, 2) for s in slot_y],
        )
        for u_z in range(2)
    }
    a, b, c = {}, {}, {}
    for u_z in (1, 0):
        a_send, a_keep, b_send, b_keep, c[u_z] = out_blocks(where[u_z], grads, got_out[u_z])
        a[u_z] = a_keep + first(a_send, X_BITS)
        b[u_z] = b_keep + first(b_send, Y_BITS)
    c = c[0] + first(c[1], Z_BITS)
    a = jnp.stack([a[u][:, :, :2] for u in range(2)]) + first(
        jnp.stack([a[u][:, :, 2:] for u in range(2)]), Y_BITS
    )
    b = b[0] + first(b[1], Z_BITS)
    c = c[:, :2] + first(c[:, 2:], X_BITS)
    a = a[0] + first(a[1], Z_BITS)
    b = b[:, :2] + first(b[:, 2:], X_BITS)
    c = c[:, :, :2] + first(c[:, :, 2:], Y_BITS)
    cube = jnp.concatenate([a, b, c], axis=3).reshape(8, BLOCK, LANES)
    cube = lax.all_to_all(cube, ALL, split_axis=0, concat_axis=0, tiled=True, axis_index_groups=cubes())
    own = inverse(inverse_out_kernel, ints(lax.rem(y, 2)), [trace, cube], False)
    inverses = lax.all_to_all(
        jnp.broadcast_to(own, (8, BLOCK, BLOCK)), ROW, split_axis=0, concat_axis=0, tiled=True
    )
    natural, total = natural_product(left, weight_grad, inverses)
    total = lax.all_to_all(total, ALL, split_axis=0, concat_axis=0, tiled=True)
    alignment = jnp.sum(total)
    return (natural * jnp.sqrt(trust_radius * D * F / alignment)).astype(jnp.bfloat16)


def solution(mesh):
    finer = Mesh(mesh.devices.reshape(mesh.shape["dp"], 2, 4, 2, 2), ALL)
    placed = (P(ALL, None), P(ALL, None), P(ROW, DP_COL))
    return jax.shard_map(
        on_device, mesh=finer, in_specs=placed, out_specs=P(ROW, DP_COL), check_vma=False
    )
```

```python
import functools
import math

import jax
import jax.numpy as jnp
from jax import lax
from jax.experimental import pallas as pl
from jax.experimental.pallas import tpu as pltpu
from jax.sharding import Mesh
from jax.sharding import PartitionSpec as P


D = 6144
F = 24576
TOKENS = 32768
BLOCK = 192
STEPS = 3
ALL = ("dp", "row_0", "row_1", "col_0", "col_1")
ROW = ("row_0", "row_1")
DP_COL = ("dp", "col_0", "col_1")

epsilon = 1e-06
damping = 0.01
trust_radius = 0.05


X_BITS = (0, 16, 2, 18)
Y_BITS = (0, 4, 8, 12)
Z_BITS = (0, 32, 64, 96)
HALF = BLOCK // 3
LANES = 128
IN_ROWS = BLOCK + 8
MIB = 1024 * 1024


def swap(array, near, far):
    return lax.ppermute(array, ALL, [(i, i ^ (far if i % 2 else near)) for i in range(128)])


def first(array, bits):
    return swap(array, bits[1], bits[3])


def second(array, bits):
    return swap(array, bits[3], bits[1])


def packed_pair(own, got, at):
    even = jnp.zeros((BLOCK, 256), jnp.float32)
    odd = jnp.zeros((BLOCK, 256), jnp.float32)
    for ref in (own, got):
        part = ref[:, at : at + 384]
        turned = part.T
        even += jnp.dot(turned[:BLOCK], part[:, :256], preferred_element_type=jnp.float32)
        odd += jnp.dot(turned[BLOCK:], part[:, 128:], preferred_element_type=jnp.float32)
    low = lax.broadcasted_iota(jnp.int32, (HALF, LANES), 1) < HALF
    e = [[even[HALF * i : HALF * (i + 1), LANES * j : LANES * (j + 1)] for j in range(2)] for i in range(3)]
    o = [[odd[HALF * i : HALF * (i + 1), LANES * j : LANES * (j + 1)] for j in range(2)] for i in range(3)]
    evens = (e[0][0], jnp.where(low, e[0][1], e[1][0]), jnp.where(low, e[2][1], e[2][0]))
    odds = (jnp.where(low, o[0][1], o[0][0]), jnp.where(low, o[1][1], o[0][1]), o[2][1])
    return evens, odds


def out_kernel(where, own, got, out):
    step = pl.program_id(0)
    for pair in range(2):
        pieces = packed_pair(own, got, pair * 384)
        for parity in range(2):
            at = 2 * pair + parity
            first = where[16 + step] + where[32 + at]
            second = where[24 + step] + where[36 + at]
            for i in range(3):
                out[first, second, HALF * i : HALF * (i + 1)] = pieces[parity][i]


def out_blocks(where, own, got):
    shape = (8, 4, BLOCK, LANES)
    return pl.pallas_call(
        out_kernel,
        grid_spec=pltpu.PrefetchScalarGridSpec(
            num_scalar_prefetch=1,
            grid=(8,),
            in_specs=[
                pl.BlockSpec((256, 768), lambda i, w: (0, w[i])),
                pl.BlockSpec((256, 768), lambda i, w: (0, w[8 + i])),
            ],
            out_specs=pl.BlockSpec(shape, lambda i, w: (0, 0, 0, 0)),
        ),
        out_shape=jax.ShapeDtypeStruct(shape, jnp.float32),
        cost_estimate=pl.CostEstimate(flops=10_000_000_000, bytes_accessed=10_000_000, transcendentals=0),
        compiler_params=pltpu.CompilerParams(vmem_limit_bytes=56 * MIB),
        name="cov_out",
    )(where, own, got)


def in_kernel(where, own, got, trace_own, trace_got, send, keep):
    y_slot = pl.program_id(0)
    u_y, v_y = y_slot // 2, lax.rem(y_slot, 2)
    trace = trace_own[...] + trace_got[...]
    for pair in range(2):
        pieces = packed_pair(own, got, pair * 384)
        for parity in range(2):
            piece = pieces[parity]
            slot = where[8 + 2 * pair + parity]

            def store(ref):
                for i in range(3):
                    ref[v_y, slot, HALF * i : HALF * (i + 1)] = piece[i]
                ref[v_y, slot, BLOCK:] = trace

            pl.when(u_y == 1)(functools.partial(store, send))
            pl.when(u_y == 0)(functools.partial(store, keep))


def in_blocks(where, own, got, trace_own, trace_got):
    shape = (2, 4, IN_ROWS, LANES)
    return pl.pallas_call(
        in_kernel,
        grid_spec=pltpu.PrefetchScalarGridSpec(
            num_scalar_prefetch=1,
            grid=(4,),
            in_specs=[
                pl.BlockSpec((256, 768), lambda i, w: (0, w[i])),
                pl.BlockSpec((256, 768), lambda i, w: (0, w[4 + i])),
                pl.BlockSpec((8, LANES), lambda i, w: (0, 0)),
                pl.BlockSpec((8, LANES), lambda i, w: (0, 0)),
            ],
            out_specs=[pl.BlockSpec(shape, lambda i, w: (0, 0, 0, 0))] * 2,
        ),
        out_shape=[jax.ShapeDtypeStruct(shape, jnp.float32)] * 2,
        cost_estimate=pl.CostEstimate(flops=5_000_000_000, bytes_accessed=5_000_000, transcendentals=0),
        compiler_params=pltpu.CompilerParams(vmem_limit_bytes=56 * MIB),
        name="cov_in",
    )(where, own, got, trace_own, trace_got)


def products_of(ref):
    value = ref[...]
    return lax.dot_general(value, value, (((1,), (1,)), ((), ())), preferred_element_type=jnp.float32)


def diagonal_rows(products):
    i = lax.broadcasted_iota(jnp.int32, (256, 256), 0)
    j = lax.broadcasted_iota(jnp.int32, (256, 256), 1)
    folded = jnp.sum(jnp.where(i == j, products, 0.0).reshape(32, 8, 256), axis=0)
    folded = folded[:, :128] + folded[:, 128:]
    return folded[:4] + folded[4:]


def tokens_kernel(where, tokens, out, total, products):
    step = pl.program_id(0)

    @pl.when(step == 0)
    def _():
        out[...] = tokens[...]
        products[...] = products_of(tokens)

    @pl.when(step == 1)
    def _():
        total[:4] = diagonal_rows(products[...] + products_of(tokens))
        total[4:] = jnp.zeros((4, LANES), jnp.float32)


def tokens_share(where, tokens):
    return pl.pallas_call(
        tokens_kernel,
        grid_spec=pltpu.PrefetchScalarGridSpec(
            num_scalar_prefetch=1,
            grid=(2,),
            in_specs=[pl.BlockSpec((256, D // 2), lambda i, w: (0, w[i]))],
            out_specs=[
                pl.BlockSpec((256, D // 2), lambda i, w: (0, 0)),
                pl.BlockSpec((8, LANES), lambda i, w: (0, 0)),
            ],
            scratch_shapes=[pltpu.VMEM((256, 256), jnp.float32)],
        ),
        out_shape=[
            jax.ShapeDtypeStruct((256, D // 2), jnp.bfloat16),
            jax.ShapeDtypeStruct((8, LANES), jnp.float32),
        ],
        cost_estimate=pl.CostEstimate(flops=500_000_000, bytes_accessed=5_000_000, transcendentals=0),
        compiler_params=pltpu.CompilerParams(vmem_limit_bytes=56 * MIB),
        name="tokens_share",
    )(where, tokens)


def grads_kernel(where, grads, before, one, two, total, products):
    step = pl.program_id(0)

    @pl.when(step == 0)
    def _():
        products[...] = jnp.zeros_like(products)

    @pl.when(step < 4)
    def _():
        one[...] = grads[...]

    @pl.when((step >= 4) & (step < 8))
    def _():
        two[...] = grads[...]

    products[...] += products_of(grads)

    @pl.when(step == 15)
    def _():
        total[:4] = before[:4]
        total[4:] = diagonal_rows(products[...])


def grads_share(where, grads, before):
    return pl.pallas_call(
        grads_kernel,
        grid_spec=pltpu.PrefetchScalarGridSpec(
            num_scalar_prefetch=1,
            grid=(16,),
            in_specs=[
                pl.BlockSpec((256, 1536), lambda i, w: (0, w[i])),
                pl.BlockSpec((8, LANES), lambda i, w: (0, 0)),
            ],
            out_specs=[
                pl.BlockSpec((256, 1536), lambda i, w: (0, jnp.minimum(i, 3))),
                pl.BlockSpec((256, 1536), lambda i, w: (0, jnp.clip(i - 4, 0, 3))),
                pl.BlockSpec((8, LANES), lambda i, w: (0, 0)),
            ],
            scratch_shapes=[pltpu.VMEM((256, 256), jnp.float32)],
        ),
        out_shape=[jax.ShapeDtypeStruct((256, 6144), jnp.bfloat16)] * 2
        + [jax.ShapeDtypeStruct((8, LANES), jnp.float32)],
        cost_estimate=pl.CostEstimate(flops=2_000_000_000, bytes_accessed=20_000_000, transcendentals=0),
        compiler_params=pltpu.CompilerParams(vmem_limit_bytes=56 * MIB),
        name="grads_share",
    )(where, grads, before)


def newton(pieces, trace, swapped, inward):
    total_in = jnp.sum(trace[:4], axis=(0, 1), keepdims=True) * (1.0 / TOKENS)
    total_out = jnp.sum(trace[4:], axis=(0, 1), keepdims=True) * (1.0 / TOKENS)
    ratio = jnp.sqrt((total_in / D + epsilon) / (total_out / F + epsilon))
    damp_root = math.sqrt(damping)
    shift = ratio * damp_root if inward else damp_root / ratio
    c = [jnp.where(swapped, pltpu.roll(value, HALF, 1), value) for value in pieces]
    t = [jnp.concatenate([value, value], axis=0).T for value in c]
    low = lax.broadcasted_iota(jnp.int32, (HALF, LANES), 1) < HALF
    zero = jnp.zeros((HALF, LANES), jnp.float32)
    rows = [
        [c[0], jnp.where(low, c[1], zero)],
        [jnp.where(low, t[0][HALF:], c[1]), jnp.where(low, t[2][HALF:], zero)],
        [jnp.where(low, t[1][:HALF], c[2]), jnp.where(low, c[2], zero)],
        [zero, zero],
    ]
    blocks = jnp.concatenate([jnp.concatenate(pair, axis=1) for pair in rows], axis=0)
    i = lax.broadcasted_iota(jnp.int32, (256, 256), 0)
    j = lax.broadcasted_iota(jnp.int32, (256, 256), 1)
    identity = jnp.where((i == j) & (i < BLOCK), 1.0, 0.0).astype(jnp.float32)
    matrix = blocks * (1.0 / TOKENS) + shift * identity
    total = jnp.sum(matrix * matrix, axis=(0, 1), keepdims=True)
    iterate = identity / jnp.sqrt(total)
    for _ in range(STEPS):
        product = jnp.dot(matrix, iterate, precision=lax.Precision.HIGHEST, preferred_element_type=jnp.float32)
        iterate = jnp.dot(
            iterate, 2.0 * identity - product, precision=lax.Precision.HIGHEST, preferred_element_type=jnp.float32
        )
    return iterate[:BLOCK, :BLOCK].astype(jnp.bfloat16)


def inverse_in_kernel(flag, one, two, out, trace_out):
    both = one[...] + two[...]
    trace = both[BLOCK:]
    trace_out[...] = trace
    pieces = [both[HALF * i : HALF * (i + 1)] for i in range(3)]
    out[...] = newton(pieces, trace, flag[0] == 1, True)


def inverse_out_kernel(flag, trace, slots, out):
    both = (slots[0] + slots[1] + (slots[2] + slots[3])) + (slots[4] + slots[5] + (slots[6] + slots[7]))
    pieces = [both[HALF * i : HALF * (i + 1)] for i in range(3)]
    value = newton(pieces, trace[...], flag[0] == 1, False)
    for i in range(8):
        out[i] = value


def inverse(kernel, flag, args, shapes):
    vmem = pl.BlockSpec(memory_space=pltpu.VMEM)
    return pl.pallas_call(
        kernel,
        in_specs=[pl.BlockSpec(memory_space=pltpu.SMEM)] + [vmem] * len(args),
        out_specs=[vmem] * len(shapes),
        out_shape=[jax.ShapeDtypeStruct(*shape) for shape in shapes],
        cost_estimate=pl.CostEstimate(flops=5_000_000_000, bytes_accessed=200_000, transcendentals=0),
    )(flag, *args)


def left_kernel(place, slots, weight, left, sums):
    for q in range(4):
        rows = slice(q * BLOCK, (q + 1) * BLOCK)
        left[rows, :] = jnp.dot(
            slots[place[q]], weight[rows, :], preferred_element_type=jnp.float32
        ).astype(jnp.bfloat16)
    for pair in range(4):
        at = 384 * pair
        turned = left[:, at : at + 384].T
        even = jnp.dot(turned[:BLOCK], weight[:, at : at + 256], preferred_element_type=jnp.float32)
        odd = jnp.dot(turned[BLOCK:], weight[:, at + 128 : at + 384], preferred_element_type=jnp.float32)
        sums[2 * pair] = even[:, :BLOCK]
        sums[2 * pair + 1] = odd[:, HALF:]


def left_product(place, slots, weight):
    vmem = pl.BlockSpec(memory_space=pltpu.VMEM)
    return pl.pallas_call(
        left_kernel,
        in_specs=[pl.BlockSpec(memory_space=pltpu.SMEM), vmem, vmem],
        out_specs=[vmem, vmem],
        out_shape=[
            jax.ShapeDtypeStruct(weight.shape, jnp.bfloat16),
            jax.ShapeDtypeStruct((8, BLOCK, BLOCK), jnp.float32),
        ],
        cost_estimate=pl.CostEstimate(flops=8_000_000_000, bytes_accessed=5_000_000, transcendentals=0),
        name="left",
    )(place, slots, weight)


def align_kernel(inverses, sums, total):
    product = jnp.zeros((BLOCK, BLOCK), jnp.float32)
    for block in range(8):
        product += inverses[block].astype(jnp.float32) * sums[block]
    total[...] = jnp.broadcast_to(jnp.sum(product, axis=(0, 1), keepdims=True), (128, LANES))


def align(inverses, sums):
    vmem = pl.BlockSpec(memory_space=pltpu.VMEM)
    return pl.pallas_call(
        align_kernel,
        in_specs=[vmem, vmem],
        out_specs=vmem,
        out_shape=jax.ShapeDtypeStruct((128, LANES), jnp.float32),
        cost_estimate=pl.CostEstimate(flops=500_000_000, bytes_accessed=1_500_000, transcendentals=0),
        name="align",
    )(inverses, sums)


def natural_kernel(left, inverses, totals, out):
    alignment = jnp.sum(totals[:, :1], axis=(0, 1), keepdims=True)
    scale = jnp.sqrt(trust_radius * D * F / alignment)
    zero = jnp.zeros((BLOCK, BLOCK), jnp.bfloat16)
    for pair in range(4):
        both = jnp.concatenate(
            [
                jnp.concatenate([inverses[2 * pair], zero], axis=1),
                jnp.concatenate([zero, inverses[2 * pair + 1]], axis=1),
            ],
            axis=0,
        )
        columns = slice(384 * pair, 384 * (pair + 1))
        natural = jnp.dot(left[:, columns], both, preferred_element_type=jnp.float32)
        out[:, columns] = (natural * scale).astype(jnp.bfloat16)


def natural_product(left, inverses, totals):
    vmem = pl.BlockSpec(memory_space=pltpu.VMEM)
    return pl.pallas_call(
        natural_kernel,
        in_specs=[vmem] * 3,
        out_specs=vmem,
        out_shape=jax.ShapeDtypeStruct(left.shape, jnp.bfloat16),
        cost_estimate=pl.CostEstimate(flops=3_000_000_000, bytes_accessed=10_000_000, transcendentals=0),
        name="natural",
    )(left, inverses, totals)


def ints(*values):
    return jnp.stack([jnp.asarray(v, jnp.int32) for v in values])


def side(far, at):
    return at // 2 if far else at % 2


def cubes(second, with_z):
    groups = {}
    for i in range(128):
        z, x_low, y, x_high, core = i // 32, i // 16 % 2, i // 4 % 4, i // 2 % 2, i % 2
        far = core == (0 if second else 1)
        axes = (z, 2 * x_high + x_low, y)
        rest = tuple(at % 2 ^ at // 2 if far else at // 2 for at in axes)
        order = tuple(side(far, at) for at in axes)
        if not with_z:
            rest, order = (z,) + rest[1:], order[1:]
        groups.setdefault((core, rest), {})[order] = i
    return [[members[k] for k in sorted(members)] for members in groups.values()]


def trade(array, groups):
    return lax.all_to_all(array, ALL, split_axis=0, concat_axis=0, tiled=True, axis_index_groups=groups)


def on_device(tokens, grads, weight_grad):
    z = lax.axis_index("dp")
    x_low = lax.axis_index("row_0")
    y = lax.axis_index("row_1")
    x_high = lax.axis_index("col_0")
    core = lax.axis_index("col_1")
    x = 2 * x_high + x_low
    other = 1 - core

    def first_of(c):
        return 1 + 2 * c

    def side_first(c, at):
        return jnp.where(c == 1, at // 2, lax.rem(at, 2))

    def side_second(c, at):
        return jnp.where(c == 0, at // 2, lax.rem(at, 2))

    def sides(c, at, to):
        mask = at ^ to
        moved = (mask == 2) | (mask == first_of(c))
        through = at ^ jnp.where(moved, first_of(c), 0)
        return side_first(c, through), side_second(c, to)

    def reached(c, at, last):
        places = []
        for through in (at, at ^ first_of(c)):
            there = side_second(c, through) == last
            places.append(jnp.where(there, through, through ^ (4 - first_of(c))))
        return places

    half, trace = tokens_share(ints(other, core), tokens)
    got_in = swap(half, 1, 1)
    chunks = [(at * 2 + h) * 2 for last in range(2) for at in reached(other, z, last) for h in range(2)]
    where = ints(*[at + other for at in chunks], *[at + core for at in chunks])
    one, two, trace = grads_share(where, grads, trace)
    got_trace = swap(trace, 1, 1)
    got_one = swap(one, 1, 1)
    got_two = swap(two, 1, 1)
    got_out = [got_one, got_two]

    x_sides = [sides(core, x, to) for to in range(4)]
    y_sides = [sides(core, y, to) for to in range(4)]

    def pair_of(u, at):
        one = at ^ (u * first_of(core))
        two = one ^ (4 - first_of(core))
        low = side_second(core, one) == 0
        return jnp.where(low, one, two), jnp.where(low, two, one)

    def relative(at, to):
        mask = at ^ to
        return ((mask == 2) | (mask == first_of(core))).astype(jnp.int32)

    y_order = [place for u in range(2) for place in pair_of(u, y)]
    where = ints(
        *[core * 4 + at for at in y_order], *y_order, *[2 * relative(x, at) + x_sides[at][1] for at in range(4)]
    )
    send, keep = in_blocks(where, tokens, got_in, trace, got_trace)
    y_side, x_side = side_second(core, y), side_second(core, x)

    def pick(array, at):
        return lax.dynamic_index_in_dim(array, at, 0, keepdims=False)

    got = first(send, Y_BITS)
    both = keep + got
    got = second(pick(both, 1 - y_side), Y_BITS)
    both = pick(both, y_side) + got
    got = first(both[2:], X_BITS)
    both = both[:2] + got
    got = second(pick(both, 1 - x_side), X_BITS)
    both = pick(both, x_side) + got
    got = first(both, Z_BITS)
    both = both + got
    got = second(both, Z_BITS)
    own, trace = inverse(
        inverse_in_kernel, ints(x_low), [both, got], [((BLOCK, BLOCK), jnp.bfloat16), ((8, LANES), jnp.float32)]
    )
    got = first(own, X_BITS)
    slots = jnp.stack([own, got])
    got = second(slots, X_BITS)
    slots = jnp.concatenate([slots, got], axis=0)
    got = swap(slots, 1, 1)
    slots = jnp.where(core == x_low, slots, got)
    g = first_of(x_low)
    order = (x, x ^ g, x ^ (4 - g), x ^ 2)
    place = ints(*[sum(jnp.where(order[s] == q, s, 0) for s in range(4)) for q in range(4)])
    left, sums = left_product(place, slots, weight_grad)

    parts = []
    for last in range(2):
        places = reached(core, z, last)
        where = ints(
            *[((at * 2 + to // 2) * 2 + core) * 2 + to % 2 for at in places for to in range(4)],
            *range(8),
            *[
                4 * side_first(core, through) + 2 * s[0]
                for through in (z, z ^ first_of(core))
                for s in x_sides
            ],
            *[2 * s[1] for _ in range(2) for s in x_sides],
            *[s[0] for s in y_sides],
            *[s[1] for s in y_sides],
        )
        blocks = out_blocks(where, grads, got_out[last])
        blocks = trade(blocks, cubes(False, True))
        parts.append(jnp.sum(blocks, axis=0))
    cube = jnp.concatenate(parts, axis=0)
    cube = trade(cube, cubes(True, True))
    (own,) = inverse(inverse_out_kernel, ints(lax.rem(y, 2)), [trace, cube], [((8, BLOCK, BLOCK), jnp.bfloat16)])
    inverses = lax.all_to_all(own, ROW, split_axis=0, concat_axis=0, tiled=True)
    total = align(inverses, sums)
    totals = lax.all_to_all(total, ALL, split_axis=0, concat_axis=0, tiled=True)
    return natural_product(left, inverses, totals)


def solution(mesh):
    finer = Mesh(mesh.devices.reshape(mesh.shape["dp"], 2, 4, 2, 2), ALL)
    placed = (P(ALL, None), P(ALL, None), P(ROW, DP_COL))
    return jax.shard_map(on_device, mesh=finer, in_specs=placed, out_specs=P(ROW, DP_COL), check_vma=False)
```

```python
import functools
import math

import jax
import jax.numpy as jnp
import numpy as np
from jax import lax
from jax.experimental import pallas as pl
from jax.experimental.pallas import tpu as pltpu
from jax.sharding import Mesh
from jax.sharding import PartitionSpec as P


D = 6144
F = 24576
TOKENS = 32768
BLOCK = 192
STEPS = 3
ALL = ("dp", "row_0", "row_1", "col_0", "col_1")
ROW = ("row_0", "row_1")
DP_COL = ("dp", "col_0", "col_1")

epsilon = 1e-06
damping = 0.01
trust_radius = 0.05


X_BITS = (0, 16, 2, 18)
Y_BITS = (0, 4, 8, 12)
Z_BITS = (0, 32, 64, 96)
HALF = BLOCK // 3
LANES = 128
IN_ROWS = BLOCK + 8
MIB = 1024 * 1024
OUT_SCALE = 2.0 ** 13 / 512.0


def swap(array, near, far):
    return lax.ppermute(array, ALL, [(i, i ^ (far if i % 2 else near)) for i in range(128)])


def first(array, bits):
    return swap(array, bits[1], bits[3])


def second(array, bits):
    return swap(array, bits[3], bits[1])


def packed_pair(own, got, at):
    even = jnp.zeros((BLOCK, 256), jnp.float32)
    odd = jnp.zeros((BLOCK, 256), jnp.float32)
    for ref in (own, got):
        part = ref[:, at : at + 384]
        turned = part.T
        even += jnp.dot(turned[:BLOCK], part[:, :256], preferred_element_type=jnp.float32)
        odd += jnp.dot(turned[BLOCK:], part[:, 128:], preferred_element_type=jnp.float32)
    low = lax.broadcasted_iota(jnp.int32, (HALF, LANES), 1) < HALF
    e = [[even[HALF * i : HALF * (i + 1), LANES * j : LANES * (j + 1)] for j in range(2)] for i in range(3)]
    o = [[odd[HALF * i : HALF * (i + 1), LANES * j : LANES * (j + 1)] for j in range(2)] for i in range(3)]
    evens = (e[0][0], jnp.where(low, e[0][1], e[1][0]), jnp.where(low, e[2][1], e[2][0]))
    odds = (jnp.where(low, o[0][1], o[0][0]), jnp.where(low, o[1][1], o[0][1]), o[2][1])
    return evens, odds


def out_kernel(index, own, got, out):
    step = pl.program_id(0)
    for pair in range(2):
        pieces = packed_pair(own, got, pair * 384)
        for parity in range(2):
            at = 2 * pair + parity
            first = index[FIRST_AT + step] + index[Y_FIRST_AT + at]
            second = index[SECOND_AT + step] + index[Y_SECOND_AT + at]
            for i in range(3):
                out[first, second, HALF * i : HALF * (i + 1)] = pieces[parity][i]


def out_blocks(index, last, own, got):
    shape = (8, 4, BLOCK, LANES)
    base = OWN_AT + 8 * last
    return pl.pallas_call(
        out_kernel,
        grid_spec=pltpu.PrefetchScalarGridSpec(
            num_scalar_prefetch=1,
            grid=(8,),
            in_specs=[
                pl.BlockSpec((256, 768), lambda i, w: (0, w[base + i])),
                pl.BlockSpec((256, 768), lambda i, w: (0, i)),
            ],
            out_specs=pl.BlockSpec(shape, lambda i, w: (0, 0, 0, 0)),
        ),
        out_shape=jax.ShapeDtypeStruct(shape, jnp.float32),
        cost_estimate=pl.CostEstimate(flops=10_000_000_000, bytes_accessed=10_000_000, transcendentals=0),
        compiler_params=pltpu.CompilerParams(vmem_limit_bytes=56 * MIB),
        name="cov_out",
    )(index, own, got)


def in_kernel(index, own, got, trace_own, trace_got, send, keep):
    slot = index[Y_SLOT_AT + pl.program_id(0)]
    trace = trace_own[...] + trace_got[...]
    for pair in range(2):
        pieces = packed_pair(own, got, pair * 384)
        for parity in range(2):
            piece = pieces[parity]
            u_x = index[X_MOVED_AT + 2 * pair + parity]
            v_x = index[X_SECOND_AT + 2 * pair + parity]

            def store(ref):
                for i in range(3):
                    ref[v_x, slot, HALF * i : HALF * (i + 1)] = piece[i]
                ref[v_x, slot, BLOCK:] = trace

            pl.when(u_x == 1)(functools.partial(store, send))
            pl.when(u_x == 0)(functools.partial(store, keep))


def in_blocks(index, own, got, trace_own, trace_got):
    shape = (2, 4, IN_ROWS, LANES)
    return pl.pallas_call(
        in_kernel,
        grid_spec=pltpu.PrefetchScalarGridSpec(
            num_scalar_prefetch=1,
            grid=(4,),
            in_specs=[
                pl.BlockSpec((256, 768), lambda i, w: (0, w[IN_AT] + i)),
                pl.BlockSpec((256, 768), lambda i, w: (0, i)),
                pl.BlockSpec((8, LANES), lambda i, w: (0, 0)),
                pl.BlockSpec((8, LANES), lambda i, w: (0, 0)),
            ],
            out_specs=[pl.BlockSpec(shape, lambda i, w: (0, 0, 0, 0))] * 2,
        ),
        out_shape=[jax.ShapeDtypeStruct(shape, jnp.float32)] * 2,
        cost_estimate=pl.CostEstimate(flops=5_000_000_000, bytes_accessed=5_000_000, transcendentals=0),
        compiler_params=pltpu.CompilerParams(vmem_limit_bytes=16 * MIB),
        name="cov_in",
    )(index, own, got, trace_own, trace_got)


def squares_of(ref):
    sums = [jnp.zeros((16, LANES), jnp.float32) for _ in range(4)]
    count = 0
    for row in range(0, ref.shape[0], 16):
        for at in range(0, ref.shape[1], LANES):
            value = ref[row : row + 16, at : at + LANES].astype(jnp.float32)
            sums[count % 4] += value * value
            count += 1
    total = (sums[0] + sums[1]) + (sums[2] + sums[3])
    total = total[:8] + total[8:]
    return total[:4] + total[4:]


def tokens_kernel(index, tokens, out, total):
    @pl.when(pl.program_id(0) == 0)
    def _():
        total[...] = jnp.zeros_like(total)

    at = pl.multiple_of(index[TOKENS_AT] * (D // 2), D // 2)
    out[...] = tokens[:, pl.ds(at, D // 2)]
    total[:4] += squares_of(tokens)


def tokens_share(index, tokens):
    return pl.pallas_call(
        tokens_kernel,
        grid_spec=pltpu.PrefetchScalarGridSpec(
            num_scalar_prefetch=1,
            grid=(4,),
            in_specs=[pl.BlockSpec((64, D), lambda i, w: (i, 0))],
            out_specs=[
                pl.BlockSpec((64, D // 2), lambda i, w: (i, 0)),
                pl.BlockSpec((8, LANES), lambda i, w: (0, 0)),
            ],
        ),
        out_shape=[
            jax.ShapeDtypeStruct((256, D // 2), jnp.bfloat16),
            jax.ShapeDtypeStruct((8, LANES), jnp.float32),
        ],
        cost_estimate=pl.CostEstimate(flops=500_000_000, bytes_accessed=5_000_000, transcendentals=0),
        compiler_params=pltpu.CompilerParams(vmem_limit_bytes=60 * MIB),
        name="tokens_share",
    )(index, tokens)


def grads_kernel(index, grads, before, one, two, total):
    @pl.when(pl.program_id(0) == 0)
    def _():
        total[...] = before[...]

    for chunk in range(4):
        for half, out in enumerate((one, two)):
            at = pl.multiple_of(index[GRADS_AT + 4 * half + chunk] * 1536, 1536)
            out[:, 1536 * chunk : 1536 * (chunk + 1)] = grads[:, pl.ds(at, 1536)]
    total[4:] += squares_of(grads)


def grads_share(index, grads, before):
    rows = 32
    return pl.pallas_call(
        grads_kernel,
        grid_spec=pltpu.PrefetchScalarGridSpec(
            num_scalar_prefetch=1,
            grid=(256 // rows,),
            in_specs=[
                pl.BlockSpec((rows, F), lambda i, w: (i, 0)),
                pl.BlockSpec((8, LANES), lambda i, w: (0, 0)),
            ],
            out_specs=[
                pl.BlockSpec((rows, 6144), lambda i, w: (i, 0)),
                pl.BlockSpec((rows, 6144), lambda i, w: (i, 0)),
                pl.BlockSpec((8, LANES), lambda i, w: (0, 0)),
            ],
        ),
        out_shape=[jax.ShapeDtypeStruct((256, 6144), jnp.bfloat16)] * 2
        + [jax.ShapeDtypeStruct((8, LANES), jnp.float32)],
        cost_estimate=pl.CostEstimate(flops=2_000_000_000, bytes_accessed=20_000_000, transcendentals=0),
        compiler_params=pltpu.CompilerParams(vmem_limit_bytes=56 * MIB),
        name="grads_share",
    )(index, grads, before)


def newton(pieces, trace, swapped, inward):
    total_in = jnp.sum(trace[:4], axis=(0, 1), keepdims=True) * (1.0 / TOKENS)
    total_out = jnp.sum(trace[4:], axis=(0, 1), keepdims=True) * (1.0 / TOKENS)
    ratio = jnp.sqrt((total_in / D + epsilon) / (total_out / F + epsilon))
    damp_root = math.sqrt(damping)
    shift = ratio * damp_root if inward else damp_root / ratio
    c = [jnp.where(swapped, pltpu.roll(value, HALF, 1), value) for value in pieces]
    t = [jnp.concatenate([value, value], axis=0).T for value in c]
    low = lax.broadcasted_iota(jnp.int32, (HALF, LANES), 1) < HALF
    zero = jnp.zeros((HALF, LANES), jnp.float32)
    rows = [
        [c[0], jnp.where(low, c[1], zero)],
        [jnp.where(low, t[0][HALF:], c[1]), jnp.where(low, t[2][HALF:], zero)],
        [jnp.where(low, t[1][:HALF], c[2]), jnp.where(low, c[2], zero)],
        [zero, zero],
    ]
    blocks = jnp.concatenate([jnp.concatenate(pair, axis=1) for pair in rows], axis=0)
    i = lax.broadcasted_iota(jnp.int32, (256, 256), 0)
    j = lax.broadcasted_iota(jnp.int32, (256, 256), 1)
    identity = jnp.where((i == j) & (i < BLOCK), 1.0, 0.0).astype(jnp.float32)
    matrix = blocks * (1.0 / TOKENS) + shift * identity
    total = jnp.sum(matrix * matrix, axis=(0, 1), keepdims=True)
    iterate = identity / jnp.sqrt(total)
    for _ in range(STEPS):
        product = jnp.dot(matrix, iterate, precision=lax.Precision.HIGHEST, preferred_element_type=jnp.float32)
        iterate = jnp.dot(
            iterate, 2.0 * identity - product, precision=lax.Precision.HIGHEST, preferred_element_type=jnp.float32
        )
    return iterate[:BLOCK, :BLOCK].astype(jnp.bfloat16)


def inverse_in_kernel(index, one, two, out, trace_out):
    both = one[...] + two[...]
    trace = both[BLOCK:]
    trace_out[...] = trace
    pieces = [both[HALF * i : HALF * (i + 1)] for i in range(3)]
    out[...] = newton(pieces, trace, index[X_LOW_AT] == 1, True)


def inverse_out_kernel(index, trace, slots, out):
    both = (slots[0] + slots[1] + (slots[2] + slots[3])) + (slots[4] + slots[5] + (slots[6] + slots[7]))
    pieces = [both[HALF * i : HALF * (i + 1)] for i in range(3)]
    value = newton(pieces, trace[...], index[Y_LOW_AT] == 1, False)
    for i in range(8):
        out[i] = value


def inverse(kernel, index, args, shapes):
    vmem = pl.BlockSpec(memory_space=pltpu.VMEM)
    return pl.pallas_call(
        kernel,
        in_specs=[pl.BlockSpec(memory_space=pltpu.SMEM)] + [vmem] * len(args),
        out_specs=[vmem] * len(shapes),
        out_shape=[jax.ShapeDtypeStruct(*shape) for shape in shapes],
        cost_estimate=pl.CostEstimate(flops=5_000_000_000, bytes_accessed=200_000, transcendentals=0),
        compiler_params=pltpu.CompilerParams(vmem_limit_bytes=16 * MIB),
    )(index, *args)


def left_kernel(index, slots, weight, left, sums):
    for q in range(4):
        rows = slice(q * BLOCK, (q + 1) * BLOCK)
        left[rows, :] = jnp.dot(
            slots[index[LEFT_AT + q]], weight[rows, :], preferred_element_type=jnp.float32
        ).astype(jnp.bfloat16)
    for pair in range(4):
        at = 384 * pair
        turned = left[:, at : at + 384].T
        even = jnp.dot(turned[:BLOCK], weight[:, at : at + 256], preferred_element_type=jnp.float32)
        odd = jnp.dot(turned[BLOCK:], weight[:, at + 128 : at + 384], preferred_element_type=jnp.float32)
        sums[2 * pair] = even[:, :BLOCK]
        sums[2 * pair + 1] = odd[:, HALF:]


def left_product(index, slots, weight):
    vmem = pl.BlockSpec(memory_space=pltpu.VMEM)
    return pl.pallas_call(
        left_kernel,
        in_specs=[pl.BlockSpec(memory_space=pltpu.SMEM), vmem, vmem],
        out_specs=[vmem, vmem],
        out_shape=[
            jax.ShapeDtypeStruct(weight.shape, jnp.bfloat16),
            jax.ShapeDtypeStruct((8, BLOCK, BLOCK), jnp.float32),
        ],
        cost_estimate=pl.CostEstimate(flops=8_000_000_000, bytes_accessed=5_000_000, transcendentals=0),
        compiler_params=pltpu.CompilerParams(vmem_limit_bytes=24 * MIB),
        name="left",
    )(index, slots, weight)


def align_kernel(inverses, sums, total):
    product = jnp.zeros((BLOCK, BLOCK), jnp.float32)
    for block in range(8):
        product += inverses[block].astype(jnp.float32) * sums[block]
    total[...] = jnp.broadcast_to(jnp.sum(product, axis=(0, 1), keepdims=True), (128, LANES))


def align(inverses, sums):
    vmem = pl.BlockSpec(memory_space=pltpu.VMEM)
    return pl.pallas_call(
        align_kernel,
        in_specs=[vmem, vmem],
        out_specs=vmem,
        out_shape=jax.ShapeDtypeStruct((128, LANES), jnp.float32),
        cost_estimate=pl.CostEstimate(flops=500_000_000, bytes_accessed=1_500_000, transcendentals=0),
        compiler_params=pltpu.CompilerParams(vmem_limit_bytes=12 * MIB),
        name="align",
    )(inverses, sums)


def natural_kernel(left, inverses, totals, out):
    alignment = jnp.sum(totals[:, :1], axis=(0, 1), keepdims=True)
    scale = jnp.sqrt(trust_radius * D * F / alignment)
    zero = jnp.zeros((BLOCK, BLOCK), jnp.bfloat16)
    for pair in range(4):
        both = jnp.concatenate(
            [
                jnp.concatenate([inverses[2 * pair], zero], axis=1),
                jnp.concatenate([zero, inverses[2 * pair + 1]], axis=1),
            ],
            axis=0,
        )
        columns = slice(384 * pair, 384 * (pair + 1))
        natural = jnp.dot(left[:, columns], both, preferred_element_type=jnp.float32)
        out[:, columns] = (natural * scale).astype(jnp.bfloat16)


def natural_product(left, inverses, totals):
    vmem = pl.BlockSpec(memory_space=pltpu.VMEM)
    return pl.pallas_call(
        natural_kernel,
        in_specs=[vmem] * 3,
        out_specs=vmem,
        out_shape=jax.ShapeDtypeStruct(left.shape, jnp.bfloat16),
        cost_estimate=pl.CostEstimate(flops=3_000_000_000, bytes_accessed=10_000_000, transcendentals=0),
        compiler_params=pltpu.CompilerParams(vmem_limit_bytes=24 * MIB),
        name="natural",
    )(left, inverses, totals)


def side(far, at):
    return at // 2 if far else at % 2


def cubes(second):
    groups = {}
    for i in range(128):
        z, x_low, y, x_high, core = i // 32, i // 16 % 2, i // 4 % 4, i // 2 % 2, i % 2
        far = core == (0 if second else 1)
        axes = (z, 2 * x_high + x_low, y)
        rest = tuple(at % 2 ^ at // 2 if far else at // 2 for at in axes)
        order = tuple(side(far, at) for at in axes)
        groups.setdefault((core, rest), {})[order] = i
    return [[members[k] for k in sorted(members)] for members in groups.values()]


def trade(array, groups):
    return lax.all_to_all(array, ALL, split_axis=0, concat_axis=0, tiled=True, axis_index_groups=groups)


TOKENS_AT, GRADS_AT, OWN_AT, FIRST_AT, SECOND_AT = 0, 4, 20, 36, 44
Y_FIRST_AT, Y_SECOND_AT, Y_SLOT_AT, X_MOVED_AT, X_SECOND_AT = 52, 56, 60, 64, 68
LEFT_AT, IN_AT, X_LOW_AT, Y_LOW_AT = 72, 76, 77, 78


def index_table():
    table = np.zeros((128, 128), np.int32)
    for i in range(128):
        z, x_low, y, x_high, core = i // 32, i // 16 % 2, i // 4 % 4, i // 2 % 2, i % 2
        x = 2 * x_high + x_low

        def reached(c, at, last):
            near = 1 + 2 * c
            return [
                through if side(c == 0, through) == last else through ^ (4 - near) for through in (at, at ^ near)
            ]

        def moved(at, to):
            return int(at ^ to in (2, 1 + 2 * core))

        def through_side(at, to):
            return side(core == 1, at ^ (moved(at, to) * (1 + 2 * core)))

        def final_side(to):
            return side(core == 0, to)

        chunks = [(at * 2 + h) * 2 for last in range(2) for at in reached(1 - core, z, last) for h in range(2)]
        order = (x, x ^ (1 + 2 * x_low), x ^ (3 - 2 * x_low), x ^ 2)
        ring = range(4)
        rows = {
            TOKENS_AT: [1 - core],
            GRADS_AT: [at + 1 - core for at in chunks],
            OWN_AT: [
                ((at * 2 + to // 2) * 2 + core) * 2 + to % 2
                for last in range(2)
                for at in reached(core, z, last)
                for to in ring
            ],
            FIRST_AT: [
                4 * side(core == 1, through) + 2 * through_side(x, to)
                for through in (z, z ^ (1 + 2 * core))
                for to in ring
            ],
            SECOND_AT: [2 * final_side(to) for to in ring] * 2,
            Y_FIRST_AT: [through_side(y, to) for to in ring],
            Y_SECOND_AT: [final_side(to) for to in ring],
            Y_SLOT_AT: [2 * moved(y, to) + final_side(to) for to in ring],
            X_MOVED_AT: [moved(x, to) for to in ring],
            X_SECOND_AT: [final_side(to) for to in ring],
            LEFT_AT: [order.index(to) for to in ring],
            IN_AT: [4 * core],
            X_LOW_AT: [x_low],
            Y_LOW_AT: [y % 2],
        }
        for start, values in rows.items():
            table[i, start : start + len(values)] = values
    return table


def on_device(tokens, grads, weight_grad):
    x_low = lax.axis_index("row_0")
    y = lax.axis_index("row_1")
    x_high = lax.axis_index("col_0")
    core = lax.axis_index("col_1")
    index = lax.dynamic_index_in_dim(jnp.asarray(index_table()), lax.axis_index(ALL), 0, keepdims=False)

    half, trace = tokens_share(index, tokens)
    got_in = swap(half, 1, 1)
    one, two, trace = grads_share(index, grads, trace)
    got_trace = swap(trace, 1, 1)
    got_one = swap(one, 1, 1)
    got_two = swap(two, 1, 1)

    def pick(array, side_of, offset):
        at = jnp.where(core == 0, side_of // 2, lax.rem(side_of, 2)) ^ offset
        return lax.dynamic_index_in_dim(array, at, 0, keepdims=False)

    x = 2 * x_high + x_low
    send, keep = in_blocks(index, tokens, got_in, trace, got_trace)
    got = first(send, X_BITS)
    both = keep + got
    got = second(pick(both, x, 1), X_BITS)
    both = pick(both, x, 0) + got
    got = first(both[2:], Y_BITS)
    both = both[:2] + got
    got = second(pick(both, y, 1), Y_BITS)
    both = pick(both, y, 0) + got
    got = first(both, Z_BITS)
    both = both + got
    got = second(both, Z_BITS)
    own, trace = inverse(
        inverse_in_kernel, index, [both, got], [((BLOCK, BLOCK), jnp.bfloat16), ((8, LANES), jnp.float32)]
    )
    got = first(own, X_BITS)
    slots = jnp.stack([own, got])
    got = second(slots, X_BITS)
    slots = jnp.concatenate([slots, got], axis=0)
    got = swap(slots, 1, 1)
    slots = jnp.where(core == x_low, slots, got)
    left, sums = left_product(index, slots, weight_grad)

    parts = []
    for last, got in enumerate((got_one, got_two)):
        blocks = out_blocks(index, last, grads, got)
        blocks = trade((blocks * OUT_SCALE).astype(jnp.float16), cubes(False))
        parts.append(jnp.sum(blocks.astype(jnp.float32), axis=0) * (1.0 / OUT_SCALE))
    cube = jnp.concatenate(parts, axis=0)
    cube = trade(cube, cubes(True))
    (own,) = inverse(inverse_out_kernel, index, [trace, cube], [((8, BLOCK, BLOCK), jnp.bfloat16)])
    inverses = lax.all_to_all(own, ROW, split_axis=0, concat_axis=0, tiled=True)
    total = align(inverses, sums)
    totals = lax.all_to_all(total, ALL, split_axis=0, concat_axis=0, tiled=True)
    return natural_product(left, inverses, totals)


def solution(mesh):
    finer = Mesh(mesh.devices.reshape(mesh.shape["dp"], 2, 4, 2, 2), ALL)
    placed = (P(ALL, None), P(ALL, None), P(ROW, DP_COL))
    return jax.shard_map(on_device, mesh=finer, in_specs=placed, out_specs=P(ROW, DP_COL), check_vma=False)
```

```python
import functools
import math

import jax
import jax.numpy as jnp
import numpy as np
from jax import lax
from jax.experimental import pallas as pl
from jax.experimental.pallas import tpu as pltpu
from jax.sharding import Mesh
from jax.sharding import PartitionSpec as P


D = 6144
F = 24576
TOKENS = 32768
BLOCK = 192
STEPS = 3
ALL = ("dp", "row_0", "row_1", "col_0", "col_1")
ROW = ("row_0", "row_1")
DP_COL = ("dp", "col_0", "col_1")

epsilon = 1e-06
damping = 0.01
trust_radius = 0.05


X_BITS = (0, 16, 2, 18)
Y_BITS = (0, 4, 8, 12)
Z_BITS = (0, 32, 64, 96)
HALF = BLOCK // 3
LANES = 128
IN_ROWS = BLOCK + 8
MIB = 1024 * 1024
OUT_SCALE = 2.0 ** 13 / 512.0


def swap(array, near, far):
    return lax.ppermute(array, ALL, [(i, i ^ (far if i % 2 else near)) for i in range(128)])


def first(array, bits):
    return swap(array, bits[1], bits[3])


def second(array, bits):
    return swap(array, bits[3], bits[1])


def packed_pair(own, got, at):
    even = jnp.zeros((BLOCK, 256), jnp.float32)
    odd = jnp.zeros((BLOCK, 256), jnp.float32)
    for ref in (own, got):
        part = ref[:, at : at + 384]
        turned = part.T
        even += jnp.dot(turned[:BLOCK], part[:, :256], preferred_element_type=jnp.float32)
        odd += jnp.dot(turned[BLOCK:], part[:, 128:], preferred_element_type=jnp.float32)
    low = lax.broadcasted_iota(jnp.int32, (HALF, LANES), 1) < HALF
    e = [[even[HALF * i : HALF * (i + 1), LANES * j : LANES * (j + 1)] for j in range(2)] for i in range(3)]
    o = [[odd[HALF * i : HALF * (i + 1), LANES * j : LANES * (j + 1)] for j in range(2)] for i in range(3)]
    evens = (e[0][0], jnp.where(low, e[0][1], e[1][0]), jnp.where(low, e[2][1], e[2][0]))
    odds = (jnp.where(low, o[0][1], o[0][0]), jnp.where(low, o[1][1], o[0][1]), o[2][1])
    return evens, odds


def out_kernel(base, index, own, got, out, own_held, got_held, own_sems, got_sems):
    step = pl.program_id(0)

    def own_copy(i):
        at = pl.multiple_of(index[base + i] * 768, 768)
        return pltpu.make_async_copy(own.at[:, pl.ds(at, 768)], own_held.at[i], own_sems.at[i])

    def got_copy(i):
        at = pl.multiple_of(i * 768, 768)
        return pltpu.make_async_copy(got.at[:, pl.ds(at, 768)], got_held.at[i], got_sems.at[i])

    @pl.when(step == 0)
    def _():
        for i in range(8):
            own_copy(i).start()
            got_copy(i).start()

    own_copy(step).wait()
    got_copy(step).wait()
    for pair in range(2):
        pieces = packed_pair(own_held.at[step], got_held.at[step], pair * 384)
        for parity in range(2):
            at = 2 * pair + parity
            first = index[FIRST_AT + step] + index[Y_FIRST_AT + at]
            second = index[SECOND_AT + step] + index[Y_SECOND_AT + at]
            for i in range(3):
                out[first, second, HALF * i : HALF * (i + 1)] = pieces[parity][i]


def out_blocks(index, last, own, got):
    shape = (8, 4, BLOCK, LANES)
    return pl.pallas_call(
        functools.partial(out_kernel, OWN_AT + 8 * last),
        grid_spec=pltpu.PrefetchScalarGridSpec(
            num_scalar_prefetch=1,
            grid=(8,),
            in_specs=[pl.BlockSpec(memory_space=pl.ANY)] * 2,
            out_specs=pl.BlockSpec(shape, lambda i, w: (0, 0, 0, 0)),
            scratch_shapes=[
                pltpu.VMEM((8, 256, 768), jnp.bfloat16),
                pltpu.VMEM((8, 256, 768), jnp.bfloat16),
                pltpu.SemaphoreType.DMA((8,)),
                pltpu.SemaphoreType.DMA((8,)),
            ],
        ),
        out_shape=jax.ShapeDtypeStruct(shape, jnp.float32),
        cost_estimate=pl.CostEstimate(flops=10_000_000_000, bytes_accessed=10_000_000, transcendentals=0),
        compiler_params=pltpu.CompilerParams(vmem_limit_bytes=54 * MIB),
        name="cov_out",
    )(index, own, got)


def in_kernel(index, own, got, trace_own, trace_got, send, keep):
    slot = index[Y_SLOT_AT + pl.program_id(0)]
    trace = trace_own[...] + trace_got[...]
    for pair in range(2):
        pieces = packed_pair(own, got, pair * 384)
        for parity in range(2):
            piece = pieces[parity]
            u_x = index[X_MOVED_AT + 2 * pair + parity]
            v_x = index[X_SECOND_AT + 2 * pair + parity]

            def store(ref):
                for i in range(3):
                    ref[v_x, slot, HALF * i : HALF * (i + 1)] = piece[i]
                ref[v_x, slot, BLOCK:] = trace

            pl.when(u_x == 1)(functools.partial(store, send))
            pl.when(u_x == 0)(functools.partial(store, keep))


def in_blocks(index, own, got, trace_own, trace_got):
    shape = (2, 4, IN_ROWS, LANES)
    return pl.pallas_call(
        in_kernel,
        grid_spec=pltpu.PrefetchScalarGridSpec(
            num_scalar_prefetch=1,
            grid=(4,),
            in_specs=[
                pl.BlockSpec((256, 768), lambda i, w: (0, w[IN_AT] + i)),
                pl.BlockSpec((256, 768), lambda i, w: (0, i)),
                pl.BlockSpec((8, LANES), lambda i, w: (0, 0)),
                pl.BlockSpec((8, LANES), lambda i, w: (0, 0)),
            ],
            out_specs=[pl.BlockSpec(shape, lambda i, w: (0, 0, 0, 0))] * 2,
        ),
        out_shape=[jax.ShapeDtypeStruct(shape, jnp.float32)] * 2,
        cost_estimate=pl.CostEstimate(flops=5_000_000_000, bytes_accessed=5_000_000, transcendentals=0),
        compiler_params=pltpu.CompilerParams(vmem_limit_bytes=16 * MIB),
        name="cov_in",
    )(index, own, got, trace_own, trace_got)


def squares_of(ref):
    sums = [jnp.zeros((16, LANES), jnp.float32) for _ in range(4)]
    count = 0
    for row in range(0, ref.shape[0], 16):
        for at in range(0, ref.shape[1], LANES):
            value = ref[row : row + 16, at : at + LANES].astype(jnp.float32)
            sums[count % 4] += value * value
            count += 1
    total = (sums[0] + sums[1]) + (sums[2] + sums[3])
    total = total[:8] + total[8:]
    return total[:4] + total[4:]


def share_kernel(chunk, first, count, index, array, *refs):
    outs, (total, held, in_sems, out_sems) = refs[:-4], refs[-4:]
    steps, rows = 8, 32
    each = count // len(outs)

    def in_copy(i):
        where = pl.ds(i * rows, rows)
        return pltpu.make_async_copy(array.at[where], held.at[where], in_sems.at[i])

    def out_copy(i, j):
        where = pl.ds(i * rows, rows)
        at = pl.multiple_of(index[first + j] * chunk, chunk)
        to = outs[j // each].at[where, pl.ds(j % each * chunk, chunk)]
        return pltpu.make_async_copy(held.at[where, pl.ds(at, chunk)], to, out_sems.at[i, j])

    for i in range(steps):
        in_copy(i).start()
    total[...] = jnp.zeros_like(total)
    for i in range(steps):
        in_copy(i).wait()
        for j in range(count):
            out_copy(i, j).start()
        total[...] += squares_of(held.at[pl.ds(i * rows, rows)])
    for i in range(steps):
        for j in range(count):
            out_copy(i, j).wait()


def share(index, array, chunk, first, count, parts):
    width = array.shape[1]
    vmem = pl.BlockSpec(memory_space=pltpu.VMEM)
    anywhere = pl.BlockSpec(memory_space=pl.ANY)
    return pl.pallas_call(
        functools.partial(share_kernel, chunk, first, count),
        in_specs=[pl.BlockSpec(memory_space=pltpu.SMEM), anywhere],
        out_specs=[anywhere] * parts + [vmem],
        out_shape=[jax.ShapeDtypeStruct((256, chunk * count // parts), jnp.bfloat16)] * parts
        + [jax.ShapeDtypeStruct((4, LANES), jnp.float32)],
        scratch_shapes=[
            pltpu.VMEM((256, width), jnp.bfloat16),
            pltpu.SemaphoreType.DMA((8,)),
            pltpu.SemaphoreType.DMA((8, count)),
        ],
        cost_estimate=pl.CostEstimate(flops=2_000_000_000, bytes_accessed=20_000_000, transcendentals=0),
        compiler_params=pltpu.CompilerParams(vmem_limit_bytes=60 * MIB),
    )(index, array)


def newton(pieces, trace, swapped, inward):
    total_in = jnp.sum(trace[:4], axis=(0, 1), keepdims=True) * (1.0 / TOKENS)
    total_out = jnp.sum(trace[4:], axis=(0, 1), keepdims=True) * (1.0 / TOKENS)
    ratio = jnp.sqrt((total_in / D + epsilon) / (total_out / F + epsilon))
    damp_root = math.sqrt(damping)
    shift = ratio * damp_root if inward else damp_root / ratio
    c = [jnp.where(swapped, pltpu.roll(value, HALF, 1), value) for value in pieces]
    t = [jnp.concatenate([value, value], axis=0).T for value in c]
    low = lax.broadcasted_iota(jnp.int32, (HALF, LANES), 1) < HALF
    zero = jnp.zeros((HALF, LANES), jnp.float32)
    rows = [
        [c[0], jnp.where(low, c[1], zero)],
        [jnp.where(low, t[0][HALF:], c[1]), jnp.where(low, t[2][HALF:], zero)],
        [jnp.where(low, t[1][:HALF], c[2]), jnp.where(low, c[2], zero)],
        [zero, zero],
    ]
    blocks = jnp.concatenate([jnp.concatenate(pair, axis=1) for pair in rows], axis=0)
    i = lax.broadcasted_iota(jnp.int32, (256, 256), 0)
    j = lax.broadcasted_iota(jnp.int32, (256, 256), 1)
    identity = jnp.where((i == j) & (i < BLOCK), 1.0, 0.0).astype(jnp.float32)
    matrix = blocks * (1.0 / TOKENS) + shift * identity
    total = jnp.sum(matrix * matrix, axis=(0, 1), keepdims=True)
    iterate = identity / jnp.sqrt(total)
    for _ in range(STEPS):
        product = jnp.dot(matrix, iterate, precision=lax.Precision.HIGHEST, preferred_element_type=jnp.float32)
        iterate = jnp.dot(
            iterate, 2.0 * identity - product, precision=lax.Precision.HIGHEST, preferred_element_type=jnp.float32
        )
    return iterate[:BLOCK, :BLOCK].astype(jnp.bfloat16)


def inverse_in_kernel(index, one, two, three, four, out, trace_out):
    both = (one[...] + three[...]) + (two[...] + four[...])
    trace = both[BLOCK:]
    trace_out[...] = trace
    pieces = [both[HALF * i : HALF * (i + 1)] for i in range(3)]
    out[...] = newton(pieces, trace, index[X_LOW_AT] == 1, True)


def inverse_out_kernel(index, trace, slots, out):
    both = (slots[0] + slots[1] + (slots[2] + slots[3])) + (slots[4] + slots[5] + (slots[6] + slots[7]))
    pieces = [both[HALF * i : HALF * (i + 1)] for i in range(3)]
    value = newton(pieces, trace[...], index[Y_LOW_AT] == 1, False)
    for i in range(8):
        out[i] = value


def inverse(kernel, index, args, shapes):
    vmem = pl.BlockSpec(memory_space=pltpu.VMEM)
    return pl.pallas_call(
        kernel,
        in_specs=[pl.BlockSpec(memory_space=pltpu.SMEM)] + [vmem] * len(args),
        out_specs=[vmem] * len(shapes),
        out_shape=[jax.ShapeDtypeStruct(*shape) for shape in shapes],
        cost_estimate=pl.CostEstimate(flops=5_000_000_000, bytes_accessed=200_000, transcendentals=0),
        compiler_params=pltpu.CompilerParams(vmem_limit_bytes=16 * MIB),
    )(index, *args)


def left_kernel(index, slots, weight, left, sums):
    for q in range(4):
        rows = slice(q * BLOCK, (q + 1) * BLOCK)
        left[rows, :] = jnp.dot(
            slots[index[LEFT_AT + q]], weight[rows, :], preferred_element_type=jnp.float32
        ).astype(jnp.bfloat16)
    for pair in range(4):
        at = 384 * pair
        turned = left[:, at : at + 384].T
        even = jnp.dot(turned[:BLOCK], weight[:, at : at + 256], preferred_element_type=jnp.float32)
        odd = jnp.dot(turned[BLOCK:], weight[:, at + 128 : at + 384], preferred_element_type=jnp.float32)
        sums[2 * pair] = even[:, :BLOCK]
        sums[2 * pair + 1] = odd[:, HALF:]


def left_product(index, slots, weight):
    vmem = pl.BlockSpec(memory_space=pltpu.VMEM)
    return pl.pallas_call(
        left_kernel,
        in_specs=[pl.BlockSpec(memory_space=pltpu.SMEM), vmem, vmem],
        out_specs=[vmem, vmem],
        out_shape=[
            jax.ShapeDtypeStruct(weight.shape, jnp.bfloat16),
            jax.ShapeDtypeStruct((8, BLOCK, BLOCK), jnp.float32),
        ],
        cost_estimate=pl.CostEstimate(flops=8_000_000_000, bytes_accessed=5_000_000, transcendentals=0),
        compiler_params=pltpu.CompilerParams(vmem_limit_bytes=24 * MIB),
        name="left",
    )(index, slots, weight)


def align_kernel(inverses, sums, total):
    product = jnp.zeros((BLOCK, BLOCK), jnp.float32)
    for block in range(8):
        product += inverses[block].astype(jnp.float32) * sums[block]
    total[...] = jnp.broadcast_to(jnp.sum(product, axis=(0, 1), keepdims=True), (128, LANES))


def align(inverses, sums):
    vmem = pl.BlockSpec(memory_space=pltpu.VMEM)
    return pl.pallas_call(
        align_kernel,
        in_specs=[vmem, vmem],
        out_specs=vmem,
        out_shape=jax.ShapeDtypeStruct((128, LANES), jnp.float32),
        cost_estimate=pl.CostEstimate(flops=500_000_000, bytes_accessed=1_500_000, transcendentals=0),
        compiler_params=pltpu.CompilerParams(vmem_limit_bytes=12 * MIB),
        name="align",
    )(inverses, sums)


def natural_kernel(left, inverses, totals, out):
    alignment = jnp.sum(totals[:, :1], axis=(0, 1), keepdims=True)
    scale = jnp.sqrt(trust_radius * D * F / alignment)
    zero = jnp.zeros((BLOCK, BLOCK), jnp.bfloat16)
    for pair in range(4):
        both = jnp.concatenate(
            [
                jnp.concatenate([inverses[2 * pair], zero], axis=1),
                jnp.concatenate([zero, inverses[2 * pair + 1]], axis=1),
            ],
            axis=0,
        )
        columns = slice(384 * pair, 384 * (pair + 1))
        natural = jnp.dot(left[:, columns], both, preferred_element_type=jnp.float32)
        out[:, columns] = (natural * scale).astype(jnp.bfloat16)


def natural_product(left, inverses, totals):
    vmem = pl.BlockSpec(memory_space=pltpu.VMEM)
    return pl.pallas_call(
        natural_kernel,
        in_specs=[vmem] * 3,
        out_specs=vmem,
        out_shape=jax.ShapeDtypeStruct(left.shape, jnp.bfloat16),
        cost_estimate=pl.CostEstimate(flops=3_000_000_000, bytes_accessed=10_000_000, transcendentals=0),
        compiler_params=pltpu.CompilerParams(vmem_limit_bytes=24 * MIB),
        name="natural",
    )(left, inverses, totals)


def side(far, at):
    return at // 2 if far else at % 2


def cubes(second):
    groups = {}
    for i in range(128):
        z, x_low, y, x_high, core = i // 32, i // 16 % 2, i // 4 % 4, i // 2 % 2, i % 2
        far = core == (0 if second else 1)
        axes = (z, 2 * x_high + x_low, y)
        rest = tuple(at % 2 ^ at // 2 if far else at // 2 for at in axes)
        order = tuple(side(far, at) for at in axes)
        groups.setdefault((core, rest), {})[order] = i
    return [[members[k] for k in sorted(members)] for members in groups.values()]


def trade(array, groups):
    return lax.all_to_all(array, ALL, split_axis=0, concat_axis=0, tiled=True, axis_index_groups=groups)


TOKENS_AT, GRADS_AT, OWN_AT, FIRST_AT, SECOND_AT = 0, 4, 20, 36, 44
Y_FIRST_AT, Y_SECOND_AT, Y_SLOT_AT, X_MOVED_AT, X_SECOND_AT = 52, 56, 60, 64, 68
LEFT_AT, IN_AT, X_LOW_AT, Y_LOW_AT = 72, 76, 77, 78


def index_table():
    table = np.zeros((128, 128), np.int32)
    for i in range(128):
        z, x_low, y, x_high, core = i // 32, i // 16 % 2, i // 4 % 4, i // 2 % 2, i % 2
        x = 2 * x_high + x_low

        def reached(c, at, last):
            near = 1 + 2 * c
            return [
                through if side(c == 0, through) == last else through ^ (4 - near) for through in (at, at ^ near)
            ]

        def moved(at, to):
            return int(at ^ to in (2, 1 + 2 * core))

        def through_side(at, to):
            return side(core == 1, at ^ (moved(at, to) * (1 + 2 * core)))

        def final_side(to):
            return side(core == 0, to)

        chunks = [(at * 2 + h) * 2 for last in range(2) for at in reached(1 - core, z, last) for h in range(2)]
        ring = range(4)
        rows = {
            TOKENS_AT: [1 - core],
            GRADS_AT: [at + 1 - core for at in chunks],
            OWN_AT: [
                ((at * 2 + to // 2) * 2 + core) * 2 + to % 2
                for last in range(2)
                for at in reached(core, z, last)
                for to in ring
            ],
            FIRST_AT: [
                4 * side(core == 1, through) + 2 * through_side(x, to)
                for through in (z, z ^ (1 + 2 * core))
                for to in ring
            ],
            SECOND_AT: [2 * final_side(to) for to in ring] * 2,
            Y_FIRST_AT: [through_side(y, to) for to in ring],
            Y_SECOND_AT: [final_side(to) for to in ring],
            Y_SLOT_AT: [y ^ to for to in ring],
            X_MOVED_AT: [moved(x, to) for to in ring],
            X_SECOND_AT: [final_side(to) for to in ring],
            LEFT_AT: [x ^ to for to in ring],
            IN_AT: [4 * core],
            X_LOW_AT: [x_low],
            Y_LOW_AT: [y % 2],
        }
        for start, values in rows.items():
            table[i, start : start + len(values)] = values
    return table


def on_device(tokens, grads, weight_grad):
    x_low = lax.axis_index("row_0")
    x_high = lax.axis_index("col_0")
    core = lax.axis_index("col_1")
    index = lax.dynamic_index_in_dim(jnp.asarray(index_table()), lax.axis_index(ALL), 0, keepdims=False)

    half, trace_in = share(index, tokens, D // 2, TOKENS_AT, 1, 1)
    got_in = swap(half, 1, 1)
    one, two, trace_out = share(index, grads, 1536, GRADS_AT, 8, 2)
    trace = jnp.concatenate([trace_in, trace_out], axis=0)
    got_trace = swap(trace, 1, 1)
    got_one = swap(one, 1, 1)
    got_two = swap(two, 1, 1)

    def pick(array, side_of, offset):
        at = jnp.where(core == 0, side_of // 2, lax.rem(side_of, 2)) ^ offset
        return lax.dynamic_index_in_dim(array, at, 0, keepdims=False)

    x = 2 * x_high + x_low
    send, keep = in_blocks(index, tokens, got_in, trace, got_trace)
    got = first(send, X_BITS)
    both = keep + got
    got = second(pick(both, x, 1), X_BITS)
    both = pick(both, x, 0) + got
    got = []
    for mask in range(1, 4):
        got.append(swap(both[mask], Y_BITS[mask], Y_BITS[mask]))
    both = (both[0] + got[1]) + (got[0] + got[2])
    got = []
    for mask in range(1, 4):
        got.append(swap(both, Z_BITS[mask], Z_BITS[mask]))
    own, trace = inverse(
        inverse_in_kernel, index, [both] + got, [((BLOCK, BLOCK), jnp.bfloat16), ((8, LANES), jnp.float32)]
    )
    slots = [own]
    for mask in range(1, 4):
        slots.append(swap(own, X_BITS[mask], X_BITS[mask]))
    slots = jnp.stack(slots)
    got = swap(slots, 1, 1)
    slots = jnp.where(core == x_low, slots, got)
    left, sums = left_product(index, slots, weight_grad)

    parts = []
    for last, got in enumerate((got_one, got_two)):
        blocks = out_blocks(index, last, grads, got)
        blocks = (blocks * OUT_SCALE).astype(jnp.float16)
        blocks = trade(blocks, cubes(False))
        parts.append(jnp.sum(blocks.astype(jnp.float32), axis=0) * (1.0 / OUT_SCALE))
    cube = jnp.concatenate(parts, axis=0)
    cube = trade(cube, cubes(True))
    (own,) = inverse(inverse_out_kernel, index, [trace, cube], [((8, BLOCK, BLOCK), jnp.bfloat16)])
    inverses = lax.all_to_all(own, ROW, split_axis=0, concat_axis=0, tiled=True)
    total = align(inverses, sums)
    totals = lax.all_to_all(total, ALL, split_axis=0, concat_axis=0, tiled=True)
    return natural_product(left, inverses, totals)


def solution(mesh):
    finer = Mesh(mesh.devices.reshape(mesh.shape["dp"], 2, 4, 2, 2), ALL)
    placed = (P(ALL, None), P(ALL, None), P(ROW, DP_COL))
    return jax.shard_map(on_device, mesh=finer, in_specs=placed, out_specs=P(ROW, DP_COL), check_vma=False)
```

```python
import functools
import math

import jax
import jax.numpy as jnp
import numpy as np
from jax import lax
from jax.experimental import pallas as pl
from jax.experimental.pallas import tpu as pltpu
from jax.sharding import Mesh
from jax.sharding import PartitionSpec as P


D = 6144
F = 24576
TOKENS = 32768
BLOCK = 192
STEPS = 3
ALL = ("dp", "row_0", "row_1", "col_0", "col_1")
ROW = ("row_0", "row_1")
DP_COL = ("dp", "col_0", "col_1")

epsilon = 1e-06
damping = 0.01
trust_radius = 0.05


X_BITS = (0, 16, 2, 18)
Y_BITS = (0, 4, 8, 12)
Z_BITS = (0, 32, 64, 96)
HALF = BLOCK // 3
LANES = 128
IN_ROWS = BLOCK + 8
MIB = 1024 * 1024
OUT_SCALE = 2.0 ** 13 / 512.0


def swap(array, near, far):
    return lax.ppermute(array, ALL, [(i, i ^ (far if i % 2 else near)) for i in range(128)])


def first(array, bits):
    return swap(array, bits[1], bits[3])


def second(array, bits):
    return swap(array, bits[3], bits[1])


def packed_pair(own, got, at):
    even = jnp.zeros((BLOCK, 256), jnp.float32)
    odd = jnp.zeros((BLOCK, 256), jnp.float32)
    for ref in (own, got):
        part = ref[:, at : at + 384]
        turned = part.T
        even += jnp.dot(turned[:BLOCK], part[:, :256], preferred_element_type=jnp.float32)
        odd += jnp.dot(turned[BLOCK:], part[:, 128:], preferred_element_type=jnp.float32)
    low = lax.broadcasted_iota(jnp.int32, (HALF, LANES), 1) < HALF
    e = [[even[HALF * i : HALF * (i + 1), LANES * j : LANES * (j + 1)] for j in range(2)] for i in range(3)]
    o = [[odd[HALF * i : HALF * (i + 1), LANES * j : LANES * (j + 1)] for j in range(2)] for i in range(3)]
    evens = (e[0][0], jnp.where(low, e[0][1], e[1][0]), jnp.where(low, e[2][1], e[2][0]))
    odds = (jnp.where(low, o[0][1], o[0][0]), jnp.where(low, o[1][1], o[0][1]), o[2][1])
    return evens, odds


def out_kernel(base, index, own, got, out, own_held, got_held, own_sems, got_sems):
    step = pl.program_id(0)

    def own_copy(i):
        at = pl.multiple_of(index[base + i] * 768, 768)
        return pltpu.make_async_copy(own.at[:, pl.ds(at, 768)], own_held.at[i], own_sems.at[i])

    def got_copy(i):
        at = pl.multiple_of(i * 768, 768)
        return pltpu.make_async_copy(got.at[:, pl.ds(at, 768)], got_held.at[i], got_sems.at[i])

    @pl.when(step == 0)
    def _():
        for i in range(8):
            own_copy(i).start()
            got_copy(i).start()

    own_copy(step).wait()
    got_copy(step).wait()
    for pair in range(2):
        pieces = packed_pair(own_held.at[step], got_held.at[step], pair * 384)
        for parity in range(2):
            at = 2 * pair + parity
            first = index[FIRST_AT + step] + index[Y_FIRST_AT + at]
            second = index[SECOND_AT + step] + index[Y_SECOND_AT + at]
            for i in range(3):
                out[first, second, HALF * i : HALF * (i + 1)] = pieces[parity][i]


def out_blocks(index, last, own, got):
    shape = (8, 4, BLOCK, LANES)
    return pl.pallas_call(
        functools.partial(out_kernel, OWN_AT + 8 * last),
        grid_spec=pltpu.PrefetchScalarGridSpec(
            num_scalar_prefetch=1,
            grid=(8,),
            in_specs=[pl.BlockSpec(memory_space=pl.ANY)] * 2,
            out_specs=pl.BlockSpec(shape, lambda i, w: (0, 0, 0, 0)),
            scratch_shapes=[
                pltpu.VMEM((8, 256, 768), jnp.bfloat16),
                pltpu.VMEM((8, 256, 768), jnp.bfloat16),
                pltpu.SemaphoreType.DMA((8,)),
                pltpu.SemaphoreType.DMA((8,)),
            ],
        ),
        out_shape=jax.ShapeDtypeStruct(shape, jnp.float32),
        cost_estimate=pl.CostEstimate(flops=10_000_000_000, bytes_accessed=10_000_000, transcendentals=0),
        compiler_params=pltpu.CompilerParams(vmem_limit_bytes=54 * MIB),
        name="cov_out",
    )(index, own, got)


def in_kernel(index, own, got, trace_own, trace_got, send, keep):
    slot = index[Y_SLOT_AT + pl.program_id(0)]
    trace = trace_own[...] + trace_got[...]
    for pair in range(2):
        pieces = packed_pair(own, got, pair * 384)
        for parity in range(2):
            piece = pieces[parity]
            u_x = index[X_MOVED_AT + 2 * pair + parity]
            v_x = index[X_SECOND_AT + 2 * pair + parity]

            def store(ref):
                for i in range(3):
                    ref[v_x, slot, HALF * i : HALF * (i + 1)] = piece[i]
                ref[v_x, slot, BLOCK:] = trace

            pl.when(u_x == 1)(functools.partial(store, send))
            pl.when(u_x == 0)(functools.partial(store, keep))


def in_blocks(index, own, got, trace_own, trace_got):
    shape = (2, 4, IN_ROWS, LANES)
    return pl.pallas_call(
        in_kernel,
        grid_spec=pltpu.PrefetchScalarGridSpec(
            num_scalar_prefetch=1,
            grid=(4,),
            in_specs=[
                pl.BlockSpec((256, 768), lambda i, w: (0, w[IN_AT] + i)),
                pl.BlockSpec((256, 768), lambda i, w: (0, i)),
                pl.BlockSpec((8, LANES), lambda i, w: (0, 0)),
                pl.BlockSpec((8, LANES), lambda i, w: (0, 0)),
            ],
            out_specs=[pl.BlockSpec(shape, lambda i, w: (0, 0, 0, 0))] * 2,
        ),
        out_shape=[jax.ShapeDtypeStruct(shape, jnp.float32)] * 2,
        cost_estimate=pl.CostEstimate(flops=5_000_000_000, bytes_accessed=5_000_000, transcendentals=0),
        compiler_params=pltpu.CompilerParams(vmem_limit_bytes=16 * MIB),
        name="cov_in",
    )(index, own, got, trace_own, trace_got)


def squares_of(ref):
    sums = [jnp.zeros((16, LANES), jnp.float32) for _ in range(4)]
    count = 0
    for row in range(0, ref.shape[0], 16):
        for at in range(0, ref.shape[1], LANES):
            value = ref[row : row + 16, at : at + LANES].astype(jnp.float32)
            sums[count % 4] += value * value
            count += 1
    total = (sums[0] + sums[1]) + (sums[2] + sums[3])
    total = total[:8] + total[8:]
    return total[:4] + total[4:]


def share_kernel(chunk, first, count, index, array, *refs):
    before, refs = (None, refs) if count == 1 else (refs[0], refs[1:])
    outs, (total, held, in_sems, out_sems) = refs[:-4], refs[-4:]
    steps, rows = 8, 32
    each = count // len(outs)

    def in_copy(i):
        where = pl.ds(i * rows, rows)
        return pltpu.make_async_copy(array.at[where], held.at[where], in_sems.at[i])

    def out_copy(i, j):
        where = pl.ds(i * rows, rows)
        at = pl.multiple_of(index[first + j] * chunk, chunk)
        to = outs[j // each].at[where, pl.ds(j % each * chunk, chunk)]
        return pltpu.make_async_copy(held.at[where, pl.ds(at, chunk)], to, out_sems.at[i, j])

    for i in range(steps):
        in_copy(i).start()
    total[:4] = jnp.zeros((4, LANES), jnp.float32) if before is None else before[4:]
    total[4:] = jnp.zeros((4, LANES), jnp.float32)
    for i in range(steps):
        in_copy(i).wait()
        for j in range(count):
            out_copy(i, j).start()
        total[4:] += squares_of(held.at[pl.ds(i * rows, rows)])
    for i in range(steps):
        for j in range(count):
            out_copy(i, j).wait()


def share(index, arrays, chunk, first, count, parts):
    width = arrays[0].shape[1]
    vmem = pl.BlockSpec(memory_space=pltpu.VMEM)
    anywhere = pl.BlockSpec(memory_space=pl.ANY)
    return pl.pallas_call(
        functools.partial(share_kernel, chunk, first, count),
        in_specs=[pl.BlockSpec(memory_space=pltpu.SMEM), anywhere, vmem][: 1 + len(arrays)],
        out_specs=[anywhere] * parts + [vmem],
        out_shape=[jax.ShapeDtypeStruct((256, chunk * count // parts), jnp.bfloat16)] * parts
        + [jax.ShapeDtypeStruct((8, LANES), jnp.float32)],
        scratch_shapes=[
            pltpu.VMEM((256, width), jnp.bfloat16),
            pltpu.SemaphoreType.DMA((8,)),
            pltpu.SemaphoreType.DMA((8, count)),
        ],
        cost_estimate=pl.CostEstimate(flops=2_000_000_000, bytes_accessed=20_000_000, transcendentals=0),
        compiler_params=pltpu.CompilerParams(vmem_limit_bytes=60 * MIB),
    )(index, *arrays)


def newton(pieces, trace, swapped, inward):
    total_in = jnp.sum(trace[:4], axis=(0, 1), keepdims=True) * (1.0 / TOKENS)
    total_out = jnp.sum(trace[4:], axis=(0, 1), keepdims=True) * (1.0 / TOKENS)
    ratio = jnp.sqrt((total_in / D + epsilon) / (total_out / F + epsilon))
    damp_root = math.sqrt(damping)
    shift = ratio * damp_root if inward else damp_root / ratio
    c = [jnp.where(swapped, pltpu.roll(value, HALF, 1), value) for value in pieces]
    t = [jnp.concatenate([value, value], axis=0).T for value in c]
    low = lax.broadcasted_iota(jnp.int32, (HALF, LANES), 1) < HALF
    zero = jnp.zeros((HALF, LANES), jnp.float32)
    rows = [
        [c[0], jnp.where(low, c[1], zero)],
        [jnp.where(low, t[0][HALF:], c[1]), jnp.where(low, t[2][HALF:], zero)],
        [jnp.where(low, t[1][:HALF], c[2]), jnp.where(low, c[2], zero)],
        [zero, zero],
    ]
    blocks = jnp.concatenate([jnp.concatenate(pair, axis=1) for pair in rows], axis=0)
    i = lax.broadcasted_iota(jnp.int32, (256, 256), 0)
    j = lax.broadcasted_iota(jnp.int32, (256, 256), 1)
    identity = jnp.where((i == j) & (i < BLOCK), 1.0, 0.0).astype(jnp.float32)
    matrix = blocks * (1.0 / TOKENS) + shift * identity
    total = jnp.sum(matrix * matrix, axis=(0, 1), keepdims=True)
    start = 1.0 / jnp.sqrt(total)
    iterate = start * (2.0 * identity - matrix * start)
    for _ in range(1, STEPS):
        product = jnp.dot(matrix, iterate, precision=lax.Precision.HIGHEST, preferred_element_type=jnp.float32)
        iterate = jnp.dot(
            iterate, 2.0 * identity - product, precision=lax.Precision.HIGHEST, preferred_element_type=jnp.float32
        )
    return iterate[:BLOCK, :BLOCK].astype(jnp.bfloat16)


def inverse_in_kernel(index, one, two, three, four, out, trace_out):
    both = (one[...] + three[...]) + (two[...] + four[...])
    trace = both[BLOCK:]
    trace_out[...] = trace
    pieces = [both[HALF * i : HALF * (i + 1)] for i in range(3)]
    out[...] = newton(pieces, trace, index[X_LOW_AT] == 1, True)


def inverse_out_kernel(index, trace, slots, out):
    both = (slots[0] + slots[1] + (slots[2] + slots[3])) + (slots[4] + slots[5] + (slots[6] + slots[7]))
    pieces = [both[HALF * i : HALF * (i + 1)] for i in range(3)]
    value = newton(pieces, trace[...], index[Y_LOW_AT] == 1, False)
    for i in range(8):
        out[i] = value


def inverse(kernel, index, args, shapes):
    vmem = pl.BlockSpec(memory_space=pltpu.VMEM)
    return pl.pallas_call(
        kernel,
        in_specs=[pl.BlockSpec(memory_space=pltpu.SMEM)] + [vmem] * len(args),
        out_specs=[vmem] * len(shapes),
        out_shape=[jax.ShapeDtypeStruct(*shape) for shape in shapes],
        cost_estimate=pl.CostEstimate(flops=5_000_000_000, bytes_accessed=200_000, transcendentals=0),
        compiler_params=pltpu.CompilerParams(vmem_limit_bytes=16 * MIB),
    )(index, *args)


def left_kernel(index, slots, weight, left, sums):
    for q in range(4):
        rows = slice(q * BLOCK, (q + 1) * BLOCK)
        left[rows, :] = jnp.dot(
            slots[index[LEFT_AT + q]], weight[rows, :], preferred_element_type=jnp.float32
        ).astype(jnp.bfloat16)
    for pair in range(4):
        at = 384 * pair
        turned = left[:, at : at + 384].T
        even = jnp.dot(turned[:BLOCK], weight[:, at : at + 256], preferred_element_type=jnp.float32)
        odd = jnp.dot(turned[BLOCK:], weight[:, at + 128 : at + 384], preferred_element_type=jnp.float32)
        sums[2 * pair] = even[:, :BLOCK]
        sums[2 * pair + 1] = odd[:, HALF:]


def left_product(index, slots, weight):
    vmem = pl.BlockSpec(memory_space=pltpu.VMEM)
    return pl.pallas_call(
        left_kernel,
        in_specs=[pl.BlockSpec(memory_space=pltpu.SMEM), vmem, vmem],
        out_specs=[vmem, vmem],
        out_shape=[
            jax.ShapeDtypeStruct(weight.shape, jnp.bfloat16),
            jax.ShapeDtypeStruct((8, BLOCK, BLOCK), jnp.float32),
        ],
        cost_estimate=pl.CostEstimate(flops=8_000_000_000, bytes_accessed=5_000_000, transcendentals=0),
        compiler_params=pltpu.CompilerParams(vmem_limit_bytes=24 * MIB),
        name="left",
    )(index, slots, weight)


def align_kernel(inverses, sums, total):
    product = jnp.zeros((BLOCK, BLOCK), jnp.float32)
    for block in range(8):
        product += inverses[block].astype(jnp.float32) * sums[block]
    total[...] = jnp.broadcast_to(jnp.sum(product, axis=(0, 1), keepdims=True), (128, LANES))


def align(inverses, sums):
    vmem = pl.BlockSpec(memory_space=pltpu.VMEM)
    return pl.pallas_call(
        align_kernel,
        in_specs=[vmem, vmem],
        out_specs=vmem,
        out_shape=jax.ShapeDtypeStruct((128, LANES), jnp.float32),
        cost_estimate=pl.CostEstimate(flops=500_000_000, bytes_accessed=1_500_000, transcendentals=0),
        compiler_params=pltpu.CompilerParams(vmem_limit_bytes=12 * MIB),
        name="align",
    )(inverses, sums)


def natural_kernel(left, inverses, totals, out):
    alignment = jnp.sum(totals[:, :1], axis=(0, 1), keepdims=True)
    scale = jnp.sqrt(trust_radius * D * F / alignment)
    zero = jnp.zeros((BLOCK, BLOCK), jnp.bfloat16)
    for pair in range(4):
        both = jnp.concatenate(
            [
                jnp.concatenate([inverses[2 * pair], zero], axis=1),
                jnp.concatenate([zero, inverses[2 * pair + 1]], axis=1),
            ],
            axis=0,
        )
        columns = slice(384 * pair, 384 * (pair + 1))
        natural = jnp.dot(left[:, columns], both, preferred_element_type=jnp.float32)
        out[:, columns] = (natural * scale).astype(jnp.bfloat16)


def natural_product(left, inverses, totals):
    vmem = pl.BlockSpec(memory_space=pltpu.VMEM)
    return pl.pallas_call(
        natural_kernel,
        in_specs=[vmem] * 3,
        out_specs=vmem,
        out_shape=jax.ShapeDtypeStruct(left.shape, jnp.bfloat16),
        cost_estimate=pl.CostEstimate(flops=3_000_000_000, bytes_accessed=10_000_000, transcendentals=0),
        compiler_params=pltpu.CompilerParams(vmem_limit_bytes=24 * MIB),
        name="natural",
    )(left, inverses, totals)


def side(far, at):
    return at // 2 if far else at % 2


def cubes(second):
    groups = {}
    for i in range(128):
        z, x_low, y, x_high, core = i // 32, i // 16 % 2, i // 4 % 4, i // 2 % 2, i % 2
        far = core == (0 if second else 1)
        axes = (z, 2 * x_high + x_low, y)
        rest = tuple(at % 2 ^ at // 2 if far else at // 2 for at in axes)
        order = tuple(side(far, at) for at in axes)
        groups.setdefault((core, rest), {})[order] = i
    return [[members[k] for k in sorted(members)] for members in groups.values()]


def trade(array, groups):
    return lax.all_to_all(array, ALL, split_axis=0, concat_axis=0, tiled=True, axis_index_groups=groups)


TOKENS_AT, GRADS_AT, OWN_AT, FIRST_AT, SECOND_AT = 0, 4, 20, 36, 44
Y_FIRST_AT, Y_SECOND_AT, Y_SLOT_AT, X_MOVED_AT, X_SECOND_AT = 52, 56, 60, 64, 68
LEFT_AT, IN_AT, X_LOW_AT, Y_LOW_AT = 72, 76, 77, 78


def index_table():
    table = np.zeros((128, 128), np.int32)
    for i in range(128):
        z, x_low, y, x_high, core = i // 32, i // 16 % 2, i // 4 % 4, i // 2 % 2, i % 2
        x = 2 * x_high + x_low

        def reached(c, at, last):
            near = 1 + 2 * c
            return [
                through if side(c == 0, through) == last else through ^ (4 - near) for through in (at, at ^ near)
            ]

        def moved(at, to):
            return int(at ^ to in (2, 1 + 2 * core))

        def through_side(at, to):
            return side(core == 1, at ^ (moved(at, to) * (1 + 2 * core)))

        def final_side(to):
            return side(core == 0, to)

        chunks = [(at * 2 + h) * 2 for last in range(2) for at in reached(1 - core, z, last) for h in range(2)]
        ring = range(4)
        rows = {
            TOKENS_AT: [1 - core],
            GRADS_AT: [at + 1 - core for at in chunks],
            OWN_AT: [
                ((at * 2 + to // 2) * 2 + core) * 2 + to % 2
                for last in range(2)
                for at in reached(core, z, last)
                for to in ring
            ],
            FIRST_AT: [
                4 * side(core == 1, through) + 2 * through_side(x, to)
                for through in (z, z ^ (1 + 2 * core))
                for to in ring
            ],
            SECOND_AT: [2 * final_side(to) for to in ring] * 2,
            Y_FIRST_AT: [through_side(y, to) for to in ring],
            Y_SECOND_AT: [final_side(to) for to in ring],
            Y_SLOT_AT: [y ^ to for to in ring],
            X_MOVED_AT: [moved(x, to) for to in ring],
            X_SECOND_AT: [final_side(to) for to in ring],
            LEFT_AT: [x ^ to for to in ring],
            IN_AT: [4 * core],
            X_LOW_AT: [x_low],
            Y_LOW_AT: [y % 2],
        }
        for start, values in rows.items():
            table[i, start : start + len(values)] = values
    return table


def on_device(tokens, grads, weight_grad):
    x_low = lax.axis_index("row_0")
    x_high = lax.axis_index("col_0")
    core = lax.axis_index("col_1")
    index = lax.dynamic_index_in_dim(jnp.asarray(index_table()), lax.axis_index(ALL), 0, keepdims=False)

    half, trace = share(index, [tokens], D // 2, TOKENS_AT, 1, 1)
    got_in = swap(half, 1, 1)
    one, two, trace = share(index, [grads, trace], 1536, GRADS_AT, 8, 2)
    got_trace = swap(trace, 1, 1)
    got_one = swap(one, 1, 1)
    got_two = swap(two, 1, 1)

    def pick(array, side_of, offset):
        at = jnp.where(core == 0, side_of // 2, lax.rem(side_of, 2)) ^ offset
        return lax.dynamic_index_in_dim(array, at, 0, keepdims=False)

    x = 2 * x_high + x_low
    send, keep = in_blocks(index, tokens, got_in, trace, got_trace)
    got = first(send, X_BITS)
    both = keep + got
    got = second(pick(both, x, 1), X_BITS)
    both = pick(both, x, 0) + got
    got = []
    for mask in range(1, 4):
        got.append(swap(both[mask], Y_BITS[mask], Y_BITS[mask]))
    both = (both[0] + got[1]) + (got[0] + got[2])
    got = []
    for mask in range(1, 4):
        got.append(swap(both, Z_BITS[mask], Z_BITS[mask]))
    own, trace = inverse(
        inverse_in_kernel, index, [both] + got, [((BLOCK, BLOCK), jnp.bfloat16), ((8, LANES), jnp.float32)]
    )
    slots = [own]
    for mask in range(1, 4):
        slots.append(swap(own, X_BITS[mask], X_BITS[mask]))
    slots = jnp.stack(slots)
    got = swap(slots, 1, 1)
    slots = jnp.where(core == x_low, slots, got)
    left, sums = left_product(index, slots, weight_grad)

    parts = []
    for last, got in enumerate((got_one, got_two)):
        blocks = out_blocks(index, last, grads, got)
        blocks = (blocks * OUT_SCALE).astype(jnp.float16)
        blocks = trade(blocks, cubes(False))
        parts.append(jnp.sum(blocks.astype(jnp.float32), axis=0) * (1.0 / OUT_SCALE))
    cube = jnp.concatenate(parts, axis=0)
    cube = trade(cube, cubes(True))
    (own,) = inverse(inverse_out_kernel, index, [trace, cube], [((8, BLOCK, BLOCK), jnp.bfloat16)])
    inverses = lax.all_to_all(own, ROW, split_axis=0, concat_axis=0, tiled=True)
    total = align(inverses, sums)
    totals = lax.all_to_all(total, ALL, split_axis=0, concat_axis=0, tiled=True)
    return natural_product(left, inverses, totals)


def solution(mesh):
    finer = Mesh(mesh.devices.reshape(mesh.shape["dp"], 2, 4, 2, 2), ALL)
    placed = (P(ALL, None), P(ALL, None), P(ROW, DP_COL))
    return jax.shard_map(on_device, mesh=finer, in_specs=placed, out_specs=P(ROW, DP_COL), check_vma=False)
```
